32 devices in a mesh: sub: 32 (over z, y, x, core).
Axes of the slice: x: 2, y: 2, z: 4, core: 2. Of those that a mesh axis runs over, the one named last changes fastest.
Arguments:
- right_side: float32 [128, 128, 512], P('sub'), may hold values from -8 to 8
- sigma: float32 [128, 128, 512], P('sub'), may hold values from 0.25 to 2
- wind: float32 [128, 128, 512], P('sub'), may hold values from -0.8 to 0.8
- local_inverse: float32 [32, 512, 512], P('sub'), may hold values from -1 to 2, as said below
- basis_y: float32 [128, 32], replicated, may hold values from -0.5 to 0.5
- basis_z: float32 [512, 64], replicated, may hold values from -0.25 to 0.25
- gamma: float32 [5, 32, 64], replicated, may hold values from 0.3 to 3
Outputs:
- solution_field: float32 [128, 128, 512], P('sub')
- residual: float32 [128, 128, 512], P('sub')
The draws below stay inside these ranges and needn't reach their ends.
Inputs may be any that keep to these rules, and one draw needn't show every extreme that they name: `local_inverse`: each block is the identity plus a perturbation whose entries lie within 2/sqrt(512) of zero; each row of the perturbation has norm about one half.
All inputs are finite; a program needn't handle non-finite values.
Results may differ from the reference program's by a relative error of at most 0.00022.
Values sent between devices are 32-bit elements; how exact they have to be, the bound alone decides.
No kernel may reach another device: no remote copies, remote signals or barrier semaphores. Data moves between devices by JAX's collectives and lax.ppermute only.
A program may use at most 64 MiB of HBM per device.

```python
import math
import jax
import jax.numpy as jnp
from jax import lax

CX = 4
NY = 128
NZ = 512
KY = 32
KZ = 64
BLOCKS = 32
NX = 128
LEVELS = 5
N_SUB = 32


def draw_local_inverse(key, part):
    noise = jnp.clip(jax.random.normal(key, (BLOCKS, NZ, NZ), jnp.float32), -4.0, 4.0)
    scaled = noise * (0.5 / jnp.sqrt(jnp.float32(NZ)))
    return scaled + jnp.eye(NZ, dtype=jnp.float32)[None]


def block_scale(own_key, shape, split, low, top_value):
    def one(axis_at, shards_of):
        steps = jax.random.uniform(jax.random.fold_in(jax.random.fold_in(own_key, 6), axis_at), (shards_of,), jnp.float32, low / len(split), top_value / len(split))
        return jnp.repeat(jnp.exp(steps), shape[axis_at] // shards_of).reshape((-1,) + (1,) * (len(shape) - axis_at - 1))

    gain = one(*split[0])
    for cut in split[1:]:
        gain = gain * one(*cut)
    return gain


def bell_draw(key, extent, deviation, reach, pieces=(), held_as=jnp.bfloat16):
    loudness = block_scale(key, extent, pieces, -0.22, 0.18) if pieces else 1.0
    result = jax.random.normal(key, extent, jnp.float32) * deviation * loudness
    return jnp.minimum(jnp.maximum(result, -reach), reach).astype(held_as)


def setup_inputs(seed: int = 0) -> dict:
    key_list = jax.random.split(jax.random.key(seed), 8)
    return {
        "right_side": bell_draw(key_list[0], (NX, NY, NZ), 1.0, 8.0, ((0, 32),), jnp.float32),
        "sigma": jnp.clip(0.25 + 1.75 * jax.random.uniform(key_list[1], (NX, NY, NZ), jnp.float32) ** block_scale(key_list[1], (NX, NY, NZ), ((0, 32),), -0.2, 0.2), 0.25, 2.0),
        "wind": jnp.clip(jax.random.uniform(key_list[2], (NX, NY, NZ), jnp.float32, -0.8, 0.8) * block_scale(key_list[2], (NX, NY, NZ), ((0, 32),), -0.4, 0.0), -0.8, 0.8),
        "local_inverse": draw_local_inverse(jax.random.fold_in(key_list[7], 71), 0),
        "basis_y": bell_draw(key_list[4], (NY, KY), NY ** -0.5, 0.5, (), jnp.float32),
        "basis_z": bell_draw(key_list[5], (NZ, KZ), NZ ** -0.5, 0.25, (), jnp.float32),
        "gamma": jnp.clip(jnp.exp(jax.random.uniform(key_list[6], (LEVELS, KY, KZ), jnp.float32, math.log(0.3), math.log(3.0))), 0.3, 3.0),
    }


HIGH = lax.Precision.HIGHEST

def apply_operator(field, sigma, wind):
    padded_x = jnp.pad(field, ((1, 1), (0, 0), (0, 0)))
    upper = padded_x[2:]
    lower = padded_x[:-2]
    padded_y = jnp.pad(field, ((0, 0), (1, 1), (0, 0)))
    padded_z = jnp.pad(field, ((0, 0), (0, 0), (1, 1)))
    beside = upper + lower + padded_y[:, 2:] + padded_y[:, :-2] + padded_z[:, :, 2:] + padded_z[:, :, :-2]
    return (6.0 + sigma) * field - beside + wind * (upper - lower)

def precondition(field, local_inverse, basis_y, basis_z, gamma):
    blocks = field.reshape(N_SUB, CX, NY, NZ)
    local = jnp.einsum('bxyz,bzw->bxyw', blocks, local_inverse, precision=HIGH)
    summed = lax.optimization_barrier(jnp.sum(blocks, axis=1))
    half = jnp.einsum('byz,zm->bym', summed, basis_z, precision=HIGH)
    proj = jnp.einsum('yk,bym->bkm', basis_y, half, precision=HIGH)
    coarse = jnp.zeros((N_SUB, KY, KZ), jnp.float32)
    for level in range(LEVELS):
        width = 2 ** (level + 1)
        grouped = lax.optimization_barrier(jnp.sum(proj.reshape(N_SUB // width, width, KY, KZ), axis=1, keepdims=True))
        grouped = jnp.broadcast_to(grouped, (N_SUB // width, width, KY, KZ)).reshape(N_SUB, KY, KZ)
        coarse = coarse + gamma[level] * grouped / jnp.sqrt(jnp.float32(CX * width))
    back = jnp.einsum('bkm,zm->bkz', coarse, basis_z, precision=HIGH)
    spread = jnp.einsum('yk,bkz->byz', basis_y, back, precision=HIGH)
    return (local + spread[:, None]).reshape(NX, NY, NZ)

def reference(right_side, sigma, wind, local_inverse, basis_y, basis_z, gamma):

    def inner(left, right):
        return jnp.sum(left * right)
    beta = jnp.sqrt(inner(right_side, right_side))
    first = right_side / beta
    z_one = precondition(first, local_inverse, basis_y, basis_z, gamma)
    image = apply_operator(z_one, sigma, wind)
    h11 = inner(first, image)
    image = image - h11 * first
    h21 = jnp.sqrt(inner(image, image))
    second = image / h21
    z_two = precondition(second, local_inverse, basis_y, basis_z, gamma)
    image = apply_operator(z_two, sigma, wind)
    h12 = inner(first, image)
    h22 = inner(second, image)
    image = image - h12 * first - h22 * second
    h32 = jnp.sqrt(inner(image, image))
    m11 = h11 * h11 + h21 * h21
    m12 = h11 * h12 + h21 * h22
    m22 = h12 * h12 + h22 * h22 + h32 * h32
    q_one = h11 * beta
    q_two = h12 * beta
    determ = m11 * m22 - m12 * m12
    y_one = (m22 * q_one - m12 * q_two) / determ
    y_two = (m11 * q_two - m12 * q_one) / determ
    solution_field = y_one * z_one + y_two * z_two
    residual = right_side - apply_operator(solution_field, sigma, wind)
    return (solution_field, residual)
```

```python
import functools
import jax
import jax.numpy as jnp
from jax import lax
from jax.experimental import pallas as pl
from jax.experimental.pallas import tpu as pltpu
from jax.sharding import PartitionSpec as P

F32 = jnp.float32
BF16 = jnp.bfloat16
AXIS = "sub"
LANES = 128
NN = (((1,), (0,)), ((), ()))
NT = (((1,), (1,)), ((), ()))
TN = (((0,), (0,)), ((), ()))


def halves(x):
    high = x.astype(BF16)
    return high, (x - high.astype(F32)).astype(BF16)


def dot3(left, right, dims=NN):
    lh, ll = left
    rh, rl = right
    mul = functools.partial(lax.dot_general, dimension_numbers=dims, preferred_element_type=F32)
    return mul(lh, rh) + (mul(lh, rl) + mul(ll, rh))


def fold_of(ky, kz):
    fold = max(1, LANES // kz)
    while ky % fold:
        fold //= 2
    return fold


def pack(block, fold):
    rows = block.shape[0] // fold
    return jnp.concatenate([block[i * rows : (i + 1) * rows] for i in range(fold)], axis=1)


def unpack(block, fold):
    cols = block.shape[1] // fold
    return jnp.concatenate([block[:, i * cols : (i + 1) * cols] for i in range(fold)], axis=0)


def project(summed, by, bz, fold):
    half = dot3(halves(summed), halves(bz))
    return pack(dot3(halves(by), halves(half), TN), fold)


def coarse_of(gath_ref, gamma_ref, tree_ref, rows, layers, fold, levels, count):
    below = None
    base = 0
    offsets = []
    for level in range(levels):
        size = count >> (level + 1)
        offsets.append(base)
        if level == 0:
            pairs = gath_ref[:, :rows, :].reshape(size, 2, rows, -1)
        else:
            pairs = below.reshape(size, 2, rows, -1)
        below = pairs[:, 0] + pairs[:, 1]
        tree_ref[pl.ds(base, size)] = below
        base += size
    scaled = [
        pack(gamma_ref[level], fold) * (1.0 / (layers * 2.0 ** (level + 1)) ** 0.5)
        for level in range(levels)
    ]
    me = lax.axis_index(AXIS)
    out = []
    for shift in (-1, 0, 1):
        who = jnp.clip(me + shift, 0, count - 1)
        total = scaled[0] * tree_ref[offsets[0] + (who >> 1)]
        for level in range(1, levels):
            total = total + scaled[level] * tree_ref[offsets[level] + (who >> (level + 1))]
        if shift:
            inside = (me + shift == who).astype(F32)
            total = total * inside
        out.append(unpack(total, fold))
    return out


def spreads(coarse, by, bz):
    ky = by.shape[1]
    back = dot3(halves(jnp.concatenate(coarse, axis=0)), halves(bz), NT)
    by_parts = halves(by)
    return [dot3(by_parts, halves(back[i * ky : (i + 1) * ky])) for i in range(len(coarse))]


def stencil(prev, here, after, sigma, wind):
    rows, depth = here.shape
    row = lax.broadcasted_iota(jnp.int32, here.shape, 0)
    col = lax.broadcasted_iota(jnp.int32, here.shape, 1)
    beside = (
        after
        + prev
        + jnp.where(row == rows - 1, 0.0, pltpu.roll(here, rows - 1, 0))
        + jnp.where(row == 0, 0.0, pltpu.roll(here, 1, 0))
        + jnp.where(col == depth - 1, 0.0, pltpu.roll(here, depth - 1, 1))
        + jnp.where(col == 0, 0.0, pltpu.roll(here, 1, 1))
    )
    return (6.0 + sigma) * here - beside + wind * (after - prev)


def lane_sum(x):
    total = jnp.sum(x, axis=0, keepdims=True)
    out = total[:, :LANES]
    for i in range(1, x.shape[1] // LANES):
        out = out + total[:, i * LANES : (i + 1) * LANES]
    return out


def full_sum(x):
    return jnp.sum(x, axis=(0, 1), keepdims=True)


def even_here():
    return lax.rem(lax.axis_index(AXIS), 2) == 0


def first_kernel(r_ref, by_ref, bz_ref, out_ref, *, fold):
    layers = r_ref.shape[0]
    summed = r_ref[0]
    for x in range(1, layers):
        summed = summed + r_ref[x]
    packed = project(summed, by_ref[...], bz_ref[...], fold)
    out_ref[...] = jnp.broadcast_to(packed[None], out_ref.shape)


def local_kernel(f_ref, inv_ref, local_ref, even_ref, odd_ref):
    layers, rows, depth = f_ref.shape
    inverse = halves(inv_ref[0])
    for x in range(layers):
        local_ref[x] = dot3(halves(f_ref[x]), inverse)
    even = even_here()
    even_ref[0] = local_ref[jnp.where(even, layers - 1, 0)]
    odd_ref[0] = local_ref[jnp.where(even, 0, layers - 1)]


def middle_kernel(
    gath_ref, local_ref, even_ref, odd_ref, r_ref, sigma_ref, wind_ref, by_ref, bz_ref, gamma_ref,
    z_ref, edge_ref, w_ref, out_ref, tree_ref, *, fold, levels, count, rows,
):
    layers = r_ref.shape[0]
    bz = bz_ref[...]
    by = by_ref[...]
    coarse = coarse_of(gath_ref, gamma_ref, tree_ref, rows, layers, fold, levels, count)
    before, own, after = spreads(coarse, by, bz)
    even = even_here().astype(F32)
    from_pair = even_ref[0]
    from_other = odd_ref[0]
    edge_ref[0] = before + (from_other * even + from_pair * (1.0 - even))
    edge_ref[1] = after + (from_pair * even + from_other * (1.0 - even))
    for x in range(layers):
        z_ref[x] = local_ref[x] + own
    rr = rw = ww = summed = None
    for x in range(layers):
        prev = edge_ref[0] if x == 0 else z_ref[x - 1]
        nxt = edge_ref[1] if x == layers - 1 else z_ref[x + 1]
        w = stencil(prev, z_ref[x], nxt, sigma_ref[x], wind_ref[x])
        w_ref[x] = w
        r = r_ref[x]
        parts = (lane_sum(r * r), lane_sum(r * w), lane_sum(w * w))
        if x == 0:
            rr, rw, ww = parts
            summed = w
        else:
            rr, rw, ww = rr + parts[0], rw + parts[1], ww + parts[2]
            summed = summed + w
    packed = project(summed, by, bz, fold)
    scalars = jnp.concatenate([rr, rw, ww, jnp.zeros((5, LANES), F32)], axis=0)
    out_ref[:, :rows, :] = jnp.broadcast_to(packed[None], (count,) + packed.shape)
    out_ref[:, rows:, :] = jnp.broadcast_to(scalars[None], (count,) + scalars.shape)


def first_scalars(gath_ref, rows):
    sums = jnp.sum(gath_ref[:, rows:, :], axis=0)
    rr = full_sum(sums[0:1])
    rw = full_sum(sums[1:2])
    ww = full_sum(sums[2:3])
    inv_rr = 1.0 / rr
    beta = jnp.sqrt(rr)
    h11 = rw * inv_rr
    h21 = jnp.sqrt(ww * inv_rr - h11 * h11)
    return beta, h11, h21


def last_kernel(
    gath_ref, local_ref, even_ref, odd_ref, r_ref, z_ref, edge_ref, w_ref, sigma_ref, wind_ref,
    by_ref, bz_ref, gamma_ref,
    z2_ref, u_ref, out_ref, tree_ref, edge2_ref, *, fold, levels, count, rows,
):
    layers = r_ref.shape[0]
    beta, h11, h21 = first_scalars(gath_ref, rows)
    scale = 1.0 / (h21 * beta)
    coarse = coarse_of(gath_ref, gamma_ref, tree_ref, rows, layers, fold, levels, count)
    before, own, after = spreads(coarse, by_ref[...], bz_ref[...])
    even = even_here().astype(F32)
    from_pair = even_ref[0]
    from_other = odd_ref[0]
    edge2_ref[0] = scale * (
        before + (from_other * even + from_pair * (1.0 - even)) - h11 * edge_ref[0]
    )
    edge2_ref[1] = scale * (
        after + (from_pair * even + from_other * (1.0 - even)) - h11 * edge_ref[1]
    )
    for x in range(layers):
        z2_ref[x] = scale * (local_ref[x] + own - h11 * z_ref[x])
    a = b = c = None
    for x in range(layers):
        prev = edge2_ref[0] if x == 0 else z2_ref[x - 1]
        nxt = edge2_ref[1] if x == layers - 1 else z2_ref[x + 1]
        u = stencil(prev, z2_ref[x], nxt, sigma_ref[x], wind_ref[x])
        u_ref[x] = u
        r = r_ref[x]
        v2 = scale * (w_ref[x] - h11 * r)
        parts = (lane_sum(r * u), lane_sum(v2 * u), lane_sum(u * u))
        a, b, c = parts if x == 0 else (a + parts[0], b + parts[1], c + parts[2])
    lane = lax.broadcasted_iota(jnp.int32, (1, LANES), 1)
    row = jnp.where(
        lane == 0, full_sum(a), jnp.where(lane == 1, full_sum(b), jnp.where(lane == 2, full_sum(c), 0.0))
    )
    out_ref[...] = jnp.broadcast_to(row, out_ref.shape)


def finish_kernel(
    sums_ref, gath_ref, r_ref, z_ref, w_ref, z2_ref, u_ref, sol_ref, res_ref, *, rows
):
    beta, h11, h21 = first_scalars(gath_ref, rows)
    sums = jnp.sum(sums_ref[...], axis=0, keepdims=True)
    lane = lax.broadcasted_iota(jnp.int32, sums.shape, 1)
    h12 = full_sum(jnp.where(lane == 0, sums, 0.0)) / beta
    h22 = full_sum(jnp.where(lane == 1, sums, 0.0))
    h32 = jnp.sqrt(full_sum(jnp.where(lane == 2, sums, 0.0)) - h12 * h12 - h22 * h22)
    m11 = h11 * h11 + h21 * h21
    m12 = h11 * h12 + h21 * h22
    m22 = h12 * h12 + h22 * h22 + h32 * h32
    q_one = h11 * beta
    q_two = h12 * beta
    determ = m11 * m22 - m12 * m12
    y_one = (m22 * q_one - m12 * q_two) / determ / beta
    y_two = (m11 * q_two - m12 * q_one) / determ
    for x in range(r_ref.shape[0]):
        sol_ref[x] = y_one * z_ref[x] + y_two * z2_ref[x]
        res_ref[x] = r_ref[x] - (y_one * w_ref[x] + y_two * u_ref[x])


def call(kernel, name, outs, args, scratch=(), flops=0):
    vmem = pl.BlockSpec(memory_space=pltpu.VMEM)
    return pl.pallas_call(
        kernel,
        name=name,
        out_shape=[jax.ShapeDtypeStruct(s, F32) for s in outs],
        in_specs=[vmem] * len(args),
        out_specs=[vmem] * len(outs),
        scratch_shapes=[pltpu.VMEM(s, F32) for s in scratch],
        compiler_params=pltpu.CompilerParams(vmem_limit_bytes=24 << 20),
        cost_estimate=pl.CostEstimate(flops=flops, bytes_accessed=0, transcendentals=0),
    )(*args)


def exchange(block):
    return lax.all_to_all(block, AXIS, 0, 0, tiled=True)


def on_device(right_side, sigma, wind, local_inverse, basis_y, basis_z, gamma):
    count = lax.axis_size(AXIS)
    levels = count.bit_length() - 1
    layers, ny, nz = right_side.shape
    ky, kz = basis_y.shape[1], basis_z.shape[1]
    fold = fold_of(ky, kz)
    rows, width = ky // fold, kz * fold
    field = (layers, ny, nz)
    edge = (1, ny, nz)
    pairs = [(i, i ^ 1) for i in range(count)]
    others = [(i, i + 1) for i in range(1, count - 1, 2)]
    others = others + [(j, i) for i, j in others]
    matmul = 6 * layers * ny * nz * nz
    sizes = dict(fold=fold, levels=levels, count=count, rows=rows)

    def local_of(f):
        local, even, odd = call(local_kernel, "local", [field, edge, edge], (f, local_inverse), flops=matmul)
        return local, lax.ppermute(even, AXIS, pairs), lax.ppermute(odd, AXIS, others)

    (sent,) = call(
        functools.partial(first_kernel, fold=fold), "first", [(count, rows, width)],
        (right_side, basis_y, basis_z), flops=matmul // 8,
    )
    gathered = exchange(sent)
    local, even, odd = local_of(right_side)
    tree = (count, rows, width)
    z, edges, w, sent = call(
        functools.partial(middle_kernel, **sizes), "middle",
        [field, (2, ny, nz), field, (count, rows + 8, width)],
        (gathered, local, even, odd, right_side, sigma, wind, basis_y, basis_z, gamma),
        [tree], flops=matmul,
    )
    gathered = exchange(sent)
    local, even, odd = local_of(w)
    z2, u, sent = call(
        functools.partial(last_kernel, **sizes), "last",
        [field, field, (count, LANES)],
        (gathered, local, even, odd, right_side, z, edges, w, sigma, wind, basis_y, basis_z, gamma),
        [tree, (2, ny, nz)], flops=matmul,
    )
    sums = exchange(sent)
    return call(
        functools.partial(finish_kernel, rows=rows), "finish", [field, field],
        (sums, gathered, right_side, z, w, z2, u), flops=matmul // 8,
    )


def solution(mesh):
    placed = (P(AXIS, None, None),) * 4 + (P(),) * 3
    return jax.shard_map(
        lambda *args: tuple(on_device(*args)),
        mesh=mesh,
        in_specs=placed,
        out_specs=(P(AXIS, None, None), P(AXIS, None, None)),
        check_vma=False,
    )
```

```python
import functools
import jax
import jax.numpy as jnp
from jax import lax
from jax.experimental import pallas as pl
from jax.experimental.pallas import tpu as pltpu
from jax.sharding import PartitionSpec as P


F32 = jnp.float32
BF16 = jnp.bfloat16
AXIS = "sub"
LANES = 128
NN = (((1,), (0,)), ((), ()))
NT = (((1,), (1,)), ((), ()))
TN = (((0,), (0,)), ((), ()))


def halves(x):
    high = x.astype(BF16)
    return high, (x - high.astype(F32)).astype(BF16)


def dot3(left, right, dims=NN):
    lh, ll = left
    rh, rl = right
    mul = functools.partial(lax.dot_general, dimension_numbers=dims, preferred_element_type=F32)
    return mul(lh, rh) + (mul(lh, rl) + mul(ll, rh))


def fold_of(ky, kz):
    fold = max(1, LANES // kz)
    while ky % fold:
        fold //= 2
    return fold


def pack(block, fold):
    rows = block.shape[0] // fold
    return jnp.concatenate([block[i * rows : (i + 1) * rows] for i in range(fold)], axis=1)


def unpack(block, fold):
    cols = block.shape[1] // fold
    return jnp.concatenate([block[:, i * cols : (i + 1) * cols] for i in range(fold)], axis=0)


def project(summed, by, bz, fold):
    half = dot3(halves(summed), halves(bz), NT)
    return pack(dot3(halves(by), halves(half)), fold)


def coarse_of(gath_ref, gamma_ref, tree_ref, rows, layers, fold, levels, count):
    below = None
    base = 0
    offsets = []
    for level in range(levels):
        size = count >> (level + 1)
        offsets.append(base)
        if level == 0:
            pairs = gath_ref[:, :rows, :].reshape(size, 2, rows, -1)
        else:
            pairs = below.reshape(size, 2, rows, -1)
        below = pairs[:, 0] + pairs[:, 1]
        tree_ref[pl.ds(base, size)] = below
        base += size
    scaled = [
        pack(gamma_ref[level], fold) * (1.0 / (layers * 2.0 ** (level + 1)) ** 0.5)
        for level in range(levels)
    ]
    me = lax.axis_index(AXIS)
    out = []
    for shift in (-1, 0, 1):
        who = jnp.clip(me + shift, 0, count - 1)
        total = scaled[0] * tree_ref[offsets[0] + (who >> 1)]
        for level in range(1, levels):
            total = total + scaled[level] * tree_ref[offsets[level] + (who >> (level + 1))]
        if shift:
            inside = (me + shift == who).astype(F32)
            total = total * inside
        out.append(unpack(total, fold))
    return out


def coarse_kernel(
    gath_ref, by_ref, bz_ref, gamma_ref, out_ref, tree_ref, *, fold, levels, count, rows, layers
):
    coarse = coarse_of(gath_ref, gamma_ref, tree_ref, rows, layers, fold, levels, count)
    ky = by_ref.shape[0]
    back = dot3(halves(jnp.concatenate(coarse, axis=0)), halves(bz_ref[...]))
    back_high, back_low = halves(back)
    by_high, by_low = halves(by_ref[...])
    left = jnp.concatenate([by_high, by_high, by_low], axis=0)
    for i in range(len(coarse)):
        high, low = (part[i * ky : (i + 1) * ky] for part in (back_high, back_low))
        right = jnp.concatenate([high, low, high], axis=0)
        out_ref[i] = lax.dot_general(left, right, TN, preferred_element_type=F32)


def stencil(prev, here, after, sigma, wind):
    rows, depth = here.shape
    row = lax.broadcasted_iota(jnp.int32, here.shape, 0)
    col = lax.broadcasted_iota(jnp.int32, here.shape, 1)
    beside = (
        after
        + prev
        + jnp.where(row == rows - 1, 0.0, pltpu.roll(here, rows - 1, 0))
        + jnp.where(row == 0, 0.0, pltpu.roll(here, 1, 0))
        + jnp.where(col == depth - 1, 0.0, pltpu.roll(here, depth - 1, 1))
        + jnp.where(col == 0, 0.0, pltpu.roll(here, 1, 1))
    )
    return (6.0 + sigma) * here - beside + wind * (after - prev)


def lane_sum(x):
    total = jnp.sum(x, axis=0, keepdims=True)
    out = total[:, :LANES]
    for i in range(1, x.shape[1] // LANES):
        out = out + total[:, i * LANES : (i + 1) * LANES]
    return out


def full_sum(x):
    return jnp.sum(x, axis=(0, 1), keepdims=True)


def even_here():
    return lax.rem(lax.axis_index(AXIS), 2) == 0


def send_edges(local_ref, even_ref, odd_ref):
    layers = local_ref.shape[0]
    even = even_here()
    even_ref[0] = local_ref[jnp.where(even, layers - 1, 0)]
    odd_ref[0] = local_ref[jnp.where(even, 0, layers - 1)]


def first_kernel(
    r_hbm, inv_hbm, by_ref, bz_ref,
    out_ref, r_ref, high_ref, low_ref, local_ref, even_ref, odd_ref,
    inv_ref, sems, *, fold,
):
    layers = r_ref.shape[0]
    loads = [pltpu.make_async_copy(r_hbm.at[x], r_ref.at[x], sems.at[x]) for x in range(layers)]
    loads.append(pltpu.make_async_copy(inv_hbm.at[0], inv_ref, sems.at[layers]))
    for load in loads:
        load.start()
    loads[0].wait()
    summed = r_ref[0]
    for x in range(1, layers):
        loads[x].wait()
        summed = summed + r_ref[x]
    packed = project(summed, by_ref[...], bz_ref[...], fold)
    out_ref[...] = jnp.broadcast_to(packed[None], out_ref.shape)
    loads[layers].wait()
    inverse = halves(inv_ref[...])
    high_ref[...], low_ref[...] = inverse
    for x in range(layers):
        local_ref[x] = dot3(halves(r_ref[x]), inverse)
    send_edges(local_ref, even_ref, odd_ref)


def middle_kernel(
    spread_ref, local_ref, even_ref, odd_ref, r_ref, sigma_ref, wind_ref, by_ref, bz_ref,
    high_ref, low_ref,
    z_ref, edge_ref, w_ref, out_ref, local2_ref, even2_ref, odd2_ref, *, fold, count, rows,
):
    layers = r_ref.shape[0]
    before, own, after = (spread_ref[i] for i in range(3))
    even = even_here().astype(F32)
    from_pair = even_ref[0]
    from_other = odd_ref[0]
    edge_ref[0] = before + (from_other * even + from_pair * (1.0 - even))
    edge_ref[1] = after + (from_pair * even + from_other * (1.0 - even))
    for x in range(layers):
        z_ref[x] = local_ref[x] + own
    rr = rw = ww = summed = None
    for x in range(layers):
        prev = edge_ref[0] if x == 0 else z_ref[x - 1]
        nxt = edge_ref[1] if x == layers - 1 else z_ref[x + 1]
        w = stencil(prev, z_ref[x], nxt, sigma_ref[x], wind_ref[x])
        w_ref[x] = w
        r = r_ref[x]
        parts = (lane_sum(r * r), lane_sum(r * w), lane_sum(w * w))
        if x == 0:
            rr, rw, ww = parts
            summed = w
        else:
            rr, rw, ww = rr + parts[0], rw + parts[1], ww + parts[2]
            summed = summed + w
    packed = project(summed, by_ref[...], bz_ref[...], fold)
    scalars = jnp.concatenate([rr, rw, ww, jnp.zeros((5, LANES), F32)], axis=0)
    out_ref[:, :rows, :] = jnp.broadcast_to(packed[None], (count,) + packed.shape)
    out_ref[:, rows:, :] = jnp.broadcast_to(scalars[None], (count,) + scalars.shape)
    inverse = (high_ref[...], low_ref[...])
    for x in range(layers):
        local2_ref[x] = dot3(halves(w_ref[x]), inverse)
    send_edges(local2_ref, even2_ref, odd2_ref)


def first_scalars(gath_ref, rows):
    sums = jnp.sum(gath_ref[:, rows:, :], axis=0)
    rr = full_sum(sums[0:1])
    rw = full_sum(sums[1:2])
    ww = full_sum(sums[2:3])
    inv_rr = 1.0 / rr
    beta = jnp.sqrt(rr)
    h11 = rw * inv_rr
    h21 = jnp.sqrt(ww * inv_rr - h11 * h11)
    return beta, h11, h21


def last_kernel(
    gath_ref, spread_ref, local_ref, even_ref, odd_ref, r_ref, z_ref, edge_ref, w_ref,
    sigma_ref, wind_ref, z2_ref, u_ref, out_ref, edge2_ref, *, rows,
):
    layers = r_ref.shape[0]
    beta, h11, h21 = first_scalars(gath_ref, rows)
    scale = 1.0 / (h21 * beta)
    before, own, after = (spread_ref[i] for i in range(3))
    even = even_here().astype(F32)
    from_pair = even_ref[0]
    from_other = odd_ref[0]
    edge2_ref[0] = scale * (
        before + (from_other * even + from_pair * (1.0 - even)) - h11 * edge_ref[0]
    )
    edge2_ref[1] = scale * (
        after + (from_pair * even + from_other * (1.0 - even)) - h11 * edge_ref[1]
    )
    for x in range(layers):
        z2_ref[x] = scale * (local_ref[x] + own - h11 * z_ref[x])
    a = b = c = None
    for x in range(layers):
        prev = edge2_ref[0] if x == 0 else z2_ref[x - 1]
        nxt = edge2_ref[1] if x == layers - 1 else z2_ref[x + 1]
        u = stencil(prev, z2_ref[x], nxt, sigma_ref[x], wind_ref[x])
        u_ref[x] = u
        r = r_ref[x]
        v2 = scale * (w_ref[x] - h11 * r)
        parts = (lane_sum(r * u), lane_sum(v2 * u), lane_sum(u * u))
        a, b, c = parts if x == 0 else (a + parts[0], b + parts[1], c + parts[2])
    lane = lax.broadcasted_iota(jnp.int32, (1, LANES), 1)
    row = jnp.where(
        lane == 0, full_sum(a), jnp.where(lane == 1, full_sum(b), jnp.where(lane == 2, full_sum(c), 0.0))
    )
    out_ref[...] = jnp.broadcast_to(row, out_ref.shape)


def finish_kernel(
    sums_ref, gath_ref, r_ref, z_ref, w_ref, z2_ref, u_ref, sol_ref, res_ref, *, rows
):
    beta, h11, h21 = first_scalars(gath_ref, rows)
    sums = jnp.sum(sums_ref[...], axis=0, keepdims=True)
    lane = lax.broadcasted_iota(jnp.int32, sums.shape, 1)
    h12 = full_sum(jnp.where(lane == 0, sums, 0.0)) / beta
    h22 = full_sum(jnp.where(lane == 1, sums, 0.0))
    h32 = jnp.sqrt(full_sum(jnp.where(lane == 2, sums, 0.0)) - h12 * h12 - h22 * h22)
    m11 = h11 * h11 + h21 * h21
    m12 = h11 * h12 + h21 * h22
    m22 = h12 * h12 + h22 * h22 + h32 * h32
    q_one = h11 * beta
    q_two = h12 * beta
    determ = m11 * m22 - m12 * m12
    y_one = (m22 * q_one - m12 * q_two) / determ / beta
    y_two = (m11 * q_two - m12 * q_one) / determ
    for x in range(r_ref.shape[0]):
        sol_ref[x] = y_one * z_ref[x] + y_two * z2_ref[x]
        res_ref[x] = r_ref[x] - (y_one * w_ref[x] + y_two * u_ref[x])


def call(kernel, outs, args, scratch=(), flops=0, hbm=()):
    vmem = pl.BlockSpec(memory_space=pltpu.VMEM)
    far = pl.BlockSpec(memory_space=pltpu.HBM)
    outs = [s if isinstance(s, jax.ShapeDtypeStruct) else jax.ShapeDtypeStruct(s, F32) for s in outs]
    return pl.pallas_call(
        kernel,
        out_shape=outs,
        in_specs=[far if i in hbm else vmem for i in range(len(args))],
        out_specs=[vmem] * len(outs),
        scratch_shapes=[pltpu.VMEM(s, F32) if isinstance(s, tuple) else s for s in scratch],
        compiler_params=pltpu.CompilerParams(vmem_limit_bytes=24 << 20),
        cost_estimate=pl.CostEstimate(flops=flops, bytes_accessed=0, transcendentals=0),
    )(*args)


def exchange(block):
    return lax.all_to_all(block, AXIS, 0, 0, tiled=True)


def on_device(right_side, sigma, wind, local_inverse, basis_y, basis_z, gamma):
    count = lax.axis_size(AXIS)
    levels = count.bit_length() - 1
    layers, ny, nz = right_side.shape
    ky, kz = basis_y.shape[1], basis_z.shape[1]
    fold = fold_of(ky, kz)
    rows, width = ky // fold, kz * fold
    field = (layers, ny, nz)
    edge = (1, ny, nz)
    square = jax.ShapeDtypeStruct((nz, nz), BF16)
    pairs = [(i, i ^ 1) for i in range(count)]
    others = [(i, i + 1) for i in range(1, count - 1, 2)]
    others = others + [(j, i) for i, j in others]
    matmul = 6 * layers * ny * nz * nz
    by, bz = basis_y.T, basis_z.T

    def round_of(sent, even, odd):
        even = lax.ppermute(even, AXIS, pairs)
        odd = lax.ppermute(odd, AXIS, others)
        gathered = exchange(sent)
        (spread,) = call(
            functools.partial(
                coarse_kernel, fold=fold, levels=levels, count=count, rows=rows, layers=layers
            ),
            [(3, ny, nz)], (gathered, by, bz, gamma), [(count, rows, width)],
            flops=matmul // 8,
        )
        return gathered, spread, even, odd

    sent, r, high, low, local, even, odd = call(
        functools.partial(first_kernel, fold=fold),
        [(count, rows, width), field, square, square, field, edge, edge],
        (right_side, local_inverse, by, bz),
        [(nz, nz), pltpu.SemaphoreType.DMA((layers + 1,))], flops=matmul, hbm=(0, 1),
    )
    _, spread, even, odd = round_of(sent, even, odd)
    z, edges, w, sent, local, even, odd = call(
        functools.partial(middle_kernel, fold=fold, count=count, rows=rows),
        [field, (2, ny, nz), field, (count, rows + 8, width), field, edge, edge],
        (spread, local, even, odd, r, sigma, wind, by, bz, high, low),
        flops=2 * matmul,
    )
    gathered, spread, even, odd = round_of(sent, even, odd)
    z2, u, sent = call(
        functools.partial(last_kernel, rows=rows),
        [field, field, (count, LANES)],
        (gathered, spread, local, even, odd, r, z, edges, w, sigma, wind),
        [(2, ny, nz)], flops=matmul,
    )
    sums = exchange(sent)
    return call(
        functools.partial(finish_kernel, rows=rows), [field, field],
        (sums, gathered, r, z, w, z2, u), flops=matmul // 8,
    )


def solution(mesh):
    placed = (P(AXIS, None, None),) * 4 + (P(),) * 3
    return jax.shard_map(
        lambda *args: tuple(on_device(*args)),
        mesh=mesh,
        in_specs=placed,
        out_specs=(P(AXIS, None, None), P(AXIS, None, None)),
        check_vma=False,
    )
```

```python
import functools
import jax
import jax.numpy as jnp
from jax import lax
from jax.experimental import pallas as pl
from jax.experimental.pallas import tpu as pltpu
from jax.sharding import PartitionSpec as P


F32 = jnp.float32
BF16 = jnp.bfloat16
AXIS = "sub"
LANES = 128
NN = (((1,), (0,)), ((), ()))
NT = (((1,), (1,)), ((), ()))
TN = (((0,), (0,)), ((), ()))


def halves(x):
    high = x.astype(BF16)
    return high, (x - high.astype(F32)).astype(BF16)


def dot3(left, right, dims=NN):
    lh, ll = left
    rh, rl = right
    mul = functools.partial(lax.dot_general, dimension_numbers=dims, preferred_element_type=F32)
    return mul(lh, rh) + (mul(lh, rl) + mul(ll, rh))


def fold_of(ky, kz):
    fold = max(1, LANES // kz)
    while ky % fold:
        fold //= 2
    return fold


def pack(block, fold):
    rows = block.shape[0] // fold
    return jnp.concatenate([block[i * rows : (i + 1) * rows] for i in range(fold)], axis=1)


def unpack(block, fold):
    cols = block.shape[1] // fold
    return jnp.concatenate([block[:, i * cols : (i + 1) * cols] for i in range(fold)], axis=0)


def project(summed, by, bz, fold):
    half = dot3(halves(summed), halves(bz), NT)
    return pack(dot3(halves(by), halves(half)), fold)


def join_kernel(got_ref, own_ref, out_ref, *, rows, width, extra):
    each = rows // 2
    first = got_ref.shape[0] - each
    both = got_ref[first:] + own_ref[first:]
    half = jnp.where(even_here(), both[:, :width], both[:, width : 2 * width])
    if not extra:
        for i in range(out_ref.shape[0] // each):
            out_ref[i * each : (i + 1) * each] = half
        return
    sums = [full_sum(both[i : i + 1, 2 * width : 2 * width + LANES]) for i in range(3)]
    lane = lax.broadcasted_iota(jnp.int32, (1, width), 1)
    row = jnp.where(
        lane == 0, sums[0], jnp.where(lane == 1, sums[1], jnp.where(lane == 2, sums[2], 0.0))
    )
    block = jnp.concatenate([half, row], axis=0)
    size = each + 1
    for i in range(out_ref.shape[0] // size):
        out_ref[i * size : (i + 1) * size] = block


def coarse_kernel(
    gath_ref, by_ref, bz_ref, gamma_ref, out_ref, tree_ref, *, fold, levels, count, rows, layers
):
    each = rows // 2
    stride = gath_ref.shape[0] // count
    for i in range(count):
        tree_ref[i // 2, (i % 2) * each : (i % 2 + 1) * each] = gath_ref[
            i * stride : i * stride + each
        ]
    offsets = [0]
    for level in range(1, levels):
        base, size = offsets[-1] + (count >> level), count >> (level + 1)
        pairs = tree_ref[offsets[-1] : base].reshape((size, 2) + tree_ref.shape[1:])
        tree_ref[base : base + size] = pairs[:, 0] + pairs[:, 1]
        offsets.append(base)
    scaled = [
        pack(gamma_ref[level], fold) * (1.0 / (layers * 2.0 ** (level + 1)) ** 0.5)
        for level in range(levels)
    ]
    me = lax.axis_index(AXIS)
    coarse = []
    for shift in (-1, 0, 1):
        who = jnp.clip(me + shift, 0, count - 1)
        total = scaled[0] * tree_ref[offsets[0] + (who >> 1)]
        for level in range(1, levels):
            total = total + scaled[level] * tree_ref[offsets[level] + (who >> (level + 1))]
        if shift:
            total = total * (me + shift == who).astype(F32)
        coarse.append(unpack(total, fold))
    ky = by_ref.shape[0]
    back = dot3(halves(jnp.concatenate(coarse, axis=0)), halves(bz_ref[...]))
    back_high, back_low = halves(back)
    by_high, by_low = halves(by_ref[...])
    left = jnp.concatenate([by_high, by_high, by_low], axis=0)
    for i in range(len(coarse)):
        high, low = (part[i * ky : (i + 1) * ky] for part in (back_high, back_low))
        right = jnp.concatenate([high, low, high], axis=0)
        out_ref[i] = lax.dot_general(left, right, TN, preferred_element_type=F32)


def stencil(prev, here, after, sigma, wind):
    rows, depth = here.shape
    row = lax.broadcasted_iota(jnp.int32, here.shape, 0)
    col = lax.broadcasted_iota(jnp.int32, here.shape, 1)
    beside = (
        after
        + prev
        + jnp.where(row == rows - 1, 0.0, pltpu.roll(here, rows - 1, 0))
        + jnp.where(row == 0, 0.0, pltpu.roll(here, 1, 0))
        + jnp.where(col == depth - 1, 0.0, pltpu.roll(here, depth - 1, 1))
        + jnp.where(col == 0, 0.0, pltpu.roll(here, 1, 1))
    )
    return (6.0 + sigma) * here - beside + wind * (after - prev)


def lane_sum(x):
    total = jnp.sum(x, axis=0, keepdims=True)
    out = total[:, :LANES]
    for i in range(1, x.shape[1] // LANES):
        out = out + total[:, i * LANES : (i + 1) * LANES]
    return out


def full_sum(x):
    return jnp.sum(x, axis=(0, 1), keepdims=True)


def even_here():
    return lax.rem(lax.axis_index(AXIS), 2) == 0


def send_edges(local_ref, pair_ref, odd_ref):
    layers, ny, _ = local_ref.shape
    even = even_here()
    pair_ref[:ny] = local_ref[jnp.where(even, layers - 1, 0)]
    odd_ref[0] = local_ref[jnp.where(even, 0, layers - 1)]


def send_proj(packed, scalars, pair_ref, ny):
    each = packed.shape[0] // 2
    parts = [packed[:each], packed[each:]]
    if scalars:
        parts.append(jnp.concatenate(scalars + [jnp.zeros((each - len(scalars), LANES), F32)], axis=0))
    used = sum(p.shape[1] for p in parts)
    if used < pair_ref.shape[1]:
        parts.append(jnp.zeros((each, pair_ref.shape[1] - used), F32))
    pair_ref[ny:] = jnp.concatenate(parts, axis=1)


def first_kernel(
    r_hbm, inv_hbm, by_ref, bz_ref,
    pair_ref, r_ref, high_ref, low_ref, local_ref, odd_ref,
    inv_ref, sems, *, fold,
):
    layers = r_ref.shape[0]
    loads = [pltpu.make_async_copy(r_hbm.at[x], r_ref.at[x], sems.at[x]) for x in range(layers)]
    loads.append(pltpu.make_async_copy(inv_hbm.at[0], inv_ref, sems.at[layers]))
    for load in loads:
        load.start()
    loads[0].wait()
    summed = r_ref[0]
    for x in range(1, layers):
        loads[x].wait()
        summed = summed + r_ref[x]
    packed = project(summed, by_ref[...], bz_ref[...], fold)
    send_proj(packed, [], pair_ref, r_ref.shape[1])
    loads[layers].wait()
    inverse = halves(inv_ref[...])
    high_ref[...], low_ref[...] = inverse
    for x in range(layers):
        local_ref[x] = dot3(halves(r_ref[x]), inverse)
    send_edges(local_ref, pair_ref, odd_ref)


def middle_kernel(
    spread_ref, local_ref, even_ref, odd_ref, r_ref, sigma_ref, wind_ref, by_ref, bz_ref,
    high_ref, low_ref,
    z_ref, edge_ref, w_ref, pair2_ref, local2_ref, odd2_ref, *, fold,
):
    layers = r_ref.shape[0]
    before, own, after = (spread_ref[i] for i in range(3))
    even = even_here().astype(F32)
    from_pair = even_ref[: r_ref.shape[1]]
    from_other = odd_ref[0]
    edge_ref[0] = before + (from_other * even + from_pair * (1.0 - even))
    edge_ref[1] = after + (from_pair * even + from_other * (1.0 - even))
    for x in range(layers):
        z_ref[x] = local_ref[x] + own
    rr = rw = ww = summed = None
    for x in range(layers):
        prev = edge_ref[0] if x == 0 else z_ref[x - 1]
        nxt = edge_ref[1] if x == layers - 1 else z_ref[x + 1]
        w = stencil(prev, z_ref[x], nxt, sigma_ref[x], wind_ref[x])
        w_ref[x] = w
        r = r_ref[x]
        parts = (lane_sum(r * r), lane_sum(r * w), lane_sum(w * w))
        if x == 0:
            rr, rw, ww = parts
            summed = w
        else:
            rr, rw, ww = rr + parts[0], rw + parts[1], ww + parts[2]
            summed = summed + w
    packed = project(summed, by_ref[...], bz_ref[...], fold)
    send_proj(packed, [rr, rw, ww], pair2_ref, r_ref.shape[1])
    inverse = (high_ref[...], low_ref[...])
    for x in range(layers):
        local2_ref[x] = dot3(halves(w_ref[x]), inverse)
    send_edges(local2_ref, pair2_ref, odd2_ref)


def lane_of(row, which):
    lane = lax.broadcasted_iota(jnp.int32, row.shape, 1)
    return full_sum(jnp.where(lane == which, row, 0.0))


def first_scalars(gath_ref, rows):
    size = rows // 2 + 1
    row = gath_ref[size - 1 : size]
    for i in range(2, gath_ref.shape[0] // size, 2):
        row = row + gath_ref[(i + 1) * size - 1 : (i + 1) * size]
    rr, rw, ww = (lane_of(row, i) for i in range(3))
    inv_rr = 1.0 / rr
    beta = jnp.sqrt(rr)
    h11 = rw * inv_rr
    h21 = jnp.sqrt(ww * inv_rr - h11 * h11)
    return beta, h11, h21


def last_kernel(
    gath_ref, spread_ref, local_ref, even_ref, odd_ref, r_ref, z_ref, edge_ref, w_ref,
    sigma_ref, wind_ref, z2_ref, u_ref, out_ref, edge2_ref, *, rows,
):
    layers = r_ref.shape[0]
    beta, h11, h21 = first_scalars(gath_ref, rows)
    scale = 1.0 / (h21 * beta)
    before, own, after = (spread_ref[i] for i in range(3))
    even = even_here().astype(F32)
    from_pair = even_ref[: r_ref.shape[1]]
    from_other = odd_ref[0]
    edge2_ref[0] = scale * (
        before + (from_other * even + from_pair * (1.0 - even)) - h11 * edge_ref[0]
    )
    edge2_ref[1] = scale * (
        after + (from_pair * even + from_other * (1.0 - even)) - h11 * edge_ref[1]
    )
    for x in range(layers):
        z2_ref[x] = scale * (local_ref[x] + own - h11 * z_ref[x])
    a = b = c = None
    for x in range(layers):
        prev = edge2_ref[0] if x == 0 else z2_ref[x - 1]
        nxt = edge2_ref[1] if x == layers - 1 else z2_ref[x + 1]
        u = stencil(prev, z2_ref[x], nxt, sigma_ref[x], wind_ref[x])
        u_ref[x] = u
        r = r_ref[x]
        v2 = scale * (w_ref[x] - h11 * r)
        parts = (lane_sum(r * u), lane_sum(v2 * u), lane_sum(u * u))
        a, b, c = parts if x == 0 else (a + parts[0], b + parts[1], c + parts[2])
    lane = lax.broadcasted_iota(jnp.int32, (1, LANES), 1)
    row = jnp.where(
        lane == 0, full_sum(a), jnp.where(lane == 1, full_sum(b), jnp.where(lane == 2, full_sum(c), 0.0))
    )
    out_ref[...] = jnp.broadcast_to(row, out_ref.shape)


def finish_kernel(
    sums_ref, gath_ref, r_ref, z_ref, w_ref, z2_ref, u_ref, sol_ref, res_ref, *, rows
):
    beta, h11, h21 = first_scalars(gath_ref, rows)
    sums = jnp.sum(sums_ref[...], axis=0, keepdims=True)
    h12 = lane_of(sums, 0) / beta
    h22 = lane_of(sums, 1)
    h32 = jnp.sqrt(lane_of(sums, 2) - h12 * h12 - h22 * h22)
    m11 = h11 * h11 + h21 * h21
    m12 = h11 * h12 + h21 * h22
    m22 = h12 * h12 + h22 * h22 + h32 * h32
    q_one = h11 * beta
    q_two = h12 * beta
    determ = m11 * m22 - m12 * m12
    y_one = (m22 * q_one - m12 * q_two) / determ / beta
    y_two = (m11 * q_two - m12 * q_one) / determ
    for x in range(r_ref.shape[0]):
        sol_ref[x] = y_one * z_ref[x] + y_two * z2_ref[x]
        res_ref[x] = r_ref[x] - (y_one * w_ref[x] + y_two * u_ref[x])


def call(kernel, outs, args, scratch=(), flops=0, hbm=()):
    vmem = pl.BlockSpec(memory_space=pltpu.VMEM)
    far = pl.BlockSpec(memory_space=pltpu.HBM)
    outs = [s if isinstance(s, jax.ShapeDtypeStruct) else jax.ShapeDtypeStruct(s, F32) for s in outs]
    return pl.pallas_call(
        kernel,
        out_shape=outs,
        in_specs=[far if i in hbm else vmem for i in range(len(args))],
        out_specs=[vmem] * len(outs),
        scratch_shapes=[pltpu.VMEM(s, F32) if isinstance(s, tuple) else s for s in scratch],
        compiler_params=pltpu.CompilerParams(vmem_limit_bytes=24 << 20),
        cost_estimate=pl.CostEstimate(flops=flops, bytes_accessed=0, transcendentals=0),
    )(*args)


def exchange(block):
    return lax.all_to_all(block, AXIS, 0, 0, tiled=True)


def on_device(right_side, sigma, wind, local_inverse, basis_y, basis_z, gamma):
    count = lax.axis_size(AXIS)
    levels = count.bit_length() - 1
    layers, ny, nz = right_side.shape
    ky, kz = basis_y.shape[1], basis_z.shape[1]
    fold = fold_of(ky, kz)
    rows, width = ky // fold, kz * fold
    field = (layers, ny, nz)
    edge = (1, ny, nz)
    square = jax.ShapeDtypeStruct((nz, nz), BF16)
    pairs = [(i, i ^ 1) for i in range(count)]
    others = [(i, i + 1) for i in range(1, count - 1, 2)]
    others = others + [(j, i) for i, j in others]
    matmul = 6 * layers * ny * nz * nz
    by, bz = basis_y.T, basis_z.T
    each = rows // 2
    pair = (ny + each, nz)

    def round_of(sent, odd, extra):
        got = lax.ppermute(sent, AXIS, pairs)
        odd = lax.ppermute(odd, AXIS, others)
        size = each + extra
        (block,) = call(
            functools.partial(join_kernel, rows=rows, width=width, extra=extra),
            [(count * size, width)], (got, sent), flops=matmul // 16,
        )
        block = exchange(block.reshape(count * size, 1, width)).reshape(count * size, width)
        (spread,) = call(
            functools.partial(
                coarse_kernel, fold=fold, levels=levels, count=count, rows=rows, layers=layers
            ),
            [(3, ny, nz)], (block, by, bz, gamma), [(count, rows, width)],
            flops=matmul // 8,
        )
        return block, spread, got, odd

    sent, r, high, low, local, odd = call(
        functools.partial(first_kernel, fold=fold),
        [pair, field, square, square, field, edge],
        (right_side, local_inverse, by, bz),
        [(nz, nz), pltpu.SemaphoreType.DMA((layers + 1,))], flops=matmul, hbm=(0, 1),
    )
    _, spread, got, odd = round_of(sent, odd, 0)
    z, edges, w, sent, local, odd = call(
        functools.partial(middle_kernel, fold=fold),
        [field, (2, ny, nz), field, pair, field, edge],
        (spread, local, got, odd, r, sigma, wind, by, bz, high, low),
        flops=2 * matmul,
    )
    gathered, spread, got, odd = round_of(sent, odd, 1)
    z2, u, sent = call(
        functools.partial(last_kernel, rows=rows),
        [field, field, (count, LANES)],
        (gathered, spread, local, got, odd, r, z, edges, w, sigma, wind),
        [(2, ny, nz)], flops=matmul,
    )
    sums = exchange(sent)
    return call(
        functools.partial(finish_kernel, rows=rows), [field, field],
        (sums, gathered, r, z, w, z2, u), flops=matmul // 8,
    )


def solution(mesh):
    placed = (P(AXIS, None, None),) * 4 + (P(),) * 3
    return jax.shard_map(
        lambda *args: tuple(on_device(*args)),
        mesh=mesh,
        in_specs=placed,
        out_specs=(P(AXIS, None, None), P(AXIS, None, None)),
        check_vma=False,
    )
```

```python
import functools
import jax
import jax.numpy as jnp
from jax import lax
from jax.experimental import pallas as pl
from jax.experimental.pallas import tpu as pltpu
from jax.sharding import PartitionSpec as P


F32 = jnp.float32
BF16 = jnp.bfloat16
AXIS = "sub"
LANES = 128
NN = (((1,), (0,)), ((), ()))
NT = (((1,), (1,)), ((), ()))
TN = (((0,), (0,)), ((), ()))
CHUNK = 16
FIRST_LIMIT = 51


def halves(x):
    high = x.astype(BF16)
    return high, (x - high.astype(F32)).astype(BF16)


def dot3(left, right, dims=NN):
    lh, ll = left
    rh, rl = right
    mul = functools.partial(lax.dot_general, dimension_numbers=dims, preferred_element_type=F32)
    return mul(lh, rh) + (mul(lh, rl) + mul(ll, rh))


def fold_of(ky, kz):
    fold = max(1, LANES // kz)
    while ky % fold:
        fold //= 2
    return fold


def pack(block, fold):
    rows = block.shape[0] // fold
    return jnp.concatenate([block[i * rows : (i + 1) * rows] for i in range(fold)], axis=1)


def unpack(block, fold):
    cols = block.shape[1] // fold
    return jnp.concatenate([block[:, i * cols : (i + 1) * cols] for i in range(fold)], axis=0)


def project(summed, by, bz, fold):
    half = dot3(halves(summed), halves(bz), NT)
    return pack(dot3(halves(by), halves(half)), fold)


def join_kernel(got_ref, own_ref, out_ref, *, rows, width, extra):
    each = rows // 2
    first = got_ref.shape[0] - each
    both = got_ref[first:] + own_ref[first:]
    half = jnp.where(even_here(), both[:, :width], both[:, width : 2 * width])
    if not extra:
        for i in range(out_ref.shape[0] // each):
            out_ref[i * each : (i + 1) * each] = half
        return
    sums = [full_sum(both[i : i + 1, 2 * width : 2 * width + LANES]) for i in range(3)]
    lane = lax.broadcasted_iota(jnp.int32, (1, width), 1)
    row = jnp.where(
        lane == 0, sums[0], jnp.where(lane == 1, sums[1], jnp.where(lane == 2, sums[2], 0.0))
    )
    block = jnp.concatenate([half, row], axis=0)
    size = each + 1
    for i in range(out_ref.shape[0] // size):
        out_ref[i * size : (i + 1) * size] = block


def coarse_kernel(
    gath_ref, by_ref, bz_ref, gamma_ref, out_ref, tree_ref, *, fold, levels, count, rows, layers
):
    each = rows // 2
    stride = gath_ref.shape[0] // count
    for i in range(count):
        tree_ref[i // 2, (i % 2) * each : (i % 2 + 1) * each] = gath_ref[
            i * stride : i * stride + each
        ]
    offsets = [0]
    for level in range(1, levels):
        base, size = offsets[-1] + (count >> level), count >> (level + 1)
        pairs = tree_ref[offsets[-1] : base].reshape((size, 2) + tree_ref.shape[1:])
        tree_ref[base : base + size] = pairs[:, 0] + pairs[:, 1]
        offsets.append(base)
    scaled = [
        pack(gamma_ref[level], fold) * (1.0 / (layers * 2.0 ** (level + 1)) ** 0.5)
        for level in range(levels)
    ]
    me = lax.axis_index(AXIS)
    coarse = []
    for shift in (-1, 0, 1):
        who = jnp.clip(me + shift, 0, count - 1)
        total = scaled[0] * tree_ref[offsets[0] + (who >> 1)]
        for level in range(1, levels):
            total = total + scaled[level] * tree_ref[offsets[level] + (who >> (level + 1))]
        if shift:
            total = total * (me + shift == who).astype(F32)
        coarse.append(unpack(total, fold))
    ky = by_ref.shape[0]
    back = dot3(halves(jnp.concatenate(coarse, axis=0)), halves(bz_ref[...]))
    back_high, back_low = halves(back)
    by_high, by_low = halves(by_ref[...])
    left = jnp.concatenate([by_high, by_high, by_low], axis=0)
    for i in range(len(coarse)):
        high, low = (part[i * ky : (i + 1) * ky] for part in (back_high, back_low))
        right = jnp.concatenate([high, low, high], axis=0)
        out_ref[i] = lax.dot_general(left, right, TN, preferred_element_type=F32)


PAD = 8


def tiles_of(ref):
    return ref.shape[-1] // LANES


def columns(j):
    return slice(j * LANES, (j + 1) * LANES)


def fill_tiles(tiled_ref, index, tile, j):
    ny = tile.shape[0]
    tiled_ref[index, j, PAD : PAD + ny] = tile


def clear_pads(tiled_ref):
    layers, tiles, full, _ = tiled_ref.shape
    zero = jnp.zeros((PAD, LANES), F32)
    for x in range(1, layers - 1):
        for j in range(tiles):
            tiled_ref[x, j, :PAD] = zero
            tiled_ref[x, j, full - PAD :] = zero


def stencil(tiled_ref, sigma_ref, wind_ref, x, first, rows, emit):
    tiles = tiled_ref.shape[1]
    lane = lax.broadcasted_iota(jnp.int32, (rows, LANES), 1)
    top = PAD + first
    here = [tiled_ref[x + 1, j, top : top + rows] for j in range(tiles)]
    up = [pltpu.roll(h, LANES - 1, 1) for h in here] + [jnp.zeros_like(here[0])]
    down = [jnp.zeros_like(here[0])] + [pltpu.roll(h, 1, 1) for h in here]
    for j in range(tiles):
        prev = tiled_ref[x, j, top : top + rows]
        after = tiled_ref[x + 2, j, top : top + rows]
        beside = (
            (after + prev)
            + (tiled_ref[x + 1, j, top - 1 : top - 1 + rows] + tiled_ref[x + 1, j, top + 1 : top + 1 + rows])
            + (
                jnp.where(lane == LANES - 1, up[j + 1], up[j])
                + jnp.where(lane == 0, down[j], down[j + 1])
            )
        )
        at = (x, slice(first, first + rows), columns(j))
        value = (6.0 + sigma_ref[at]) * here[j] - beside + wind_ref[at] * (after - prev)
        emit(at, value)


def rows_sum(x):
    return jnp.sum(x.reshape(x.shape[0] // 8, 8, LANES), axis=0)


def full_sum(x):
    return jnp.sum(x, axis=(0, 1), keepdims=True)


def even_here():
    return lax.rem(lax.axis_index(AXIS), 2) == 0


def send_edges(local_ref, pair_ref, odd_ref):
    layers, ny, _ = local_ref.shape
    even = even_here()
    pair_ref[:ny] = local_ref[jnp.where(even, layers - 1, 0)]
    odd_ref[0] = local_ref[jnp.where(even, 0, layers - 1)]


def send_proj(packed, scalars, pair_ref, ny):
    each = packed.shape[0] // 2
    parts = [packed[:each], packed[each:]]
    if scalars:
        parts.append(jnp.concatenate(scalars + [jnp.zeros((each - len(scalars), LANES), F32)], axis=0))
    used = sum(p.shape[1] for p in parts)
    if used < pair_ref.shape[1]:
        parts.append(jnp.zeros((each, pair_ref.shape[1] - used), F32))
    pair_ref[ny:] = jnp.concatenate(parts, axis=1)


def first_kernel(
    r_hbm, inv_hbm, local_ref, summed_ref, odd_ref, high_ref, low_ref, rr_ref, r_ref, inv_ref, sems
):
    layers, _, _ = r_ref.shape
    moves = [(r_hbm.at[x], r_ref.at[x]) for x in range(layers)] + [(inv_hbm.at[0], inv_ref)]
    loads = [pltpu.make_async_copy(*move, sems.at[i]) for i, move in enumerate(moves)]
    for load in loads:
        load.start()
    for load in loads[:layers]:
        load.wait()
    total = jnp.zeros((8, LANES), F32)
    for j in range(tiles_of(r_ref)):
        summed = None
        for x in range(layers):
            r = r_ref[x, :, columns(j)]
            total = total + rows_sum(r * r)
            summed = r if x == 0 else summed + r
        summed_ref[:, columns(j)] = summed
    rr_ref[:8] = total
    loads[layers].wait()
    inverse = halves(inv_ref[...])
    high_ref[...], low_ref[...] = inverse
    for x in range(layers):
        local_ref[x] = dot3(halves(r_ref[x]), inverse)
    odd_ref[0] = local_ref[jnp.where(even_here(), 0, layers - 1)]


def project_kernel(summed_ref, local_ref, by_ref, bz_ref, pair_ref, *, fold):
    layers, ny, _ = local_ref.shape
    pair_ref[:ny] = local_ref[jnp.where(even_here(), layers - 1, 0)]
    send_proj(project(summed_ref[...], by_ref[...], bz_ref[...], fold), [], pair_ref, ny)


def halo_of(even_ref, odd_ref, j):
    ny = odd_ref.shape[1]
    even = even_here()
    pair = even_ref[:ny, columns(j)]
    odd = odd_ref[0, :, columns(j)]
    return jnp.where(even, odd, pair), jnp.where(even, pair, odd)


def middle_kernel(
    spread_ref, local_ref, even_ref, odd_ref, r_ref, sigma_ref, wind_ref, by_ref, bz_ref,
    high_ref, low_ref, rr_ref,
    z_ref, w_ref, pair2_ref, local2_ref, odd2_ref, *, fold,
):
    layers, ny, _ = r_ref.shape
    clear_pads(z_ref)
    for j in range(tiles_of(r_ref)):
        before, after = halo_of(even_ref, odd_ref, j)
        fill_tiles(z_ref, 0, spread_ref[0, :, columns(j)] + before, j)
        fill_tiles(z_ref, layers + 1, spread_ref[2, :, columns(j)] + after, j)
        own = spread_ref[1, :, columns(j)]
        for x in range(layers):
            fill_tiles(z_ref, x + 1, local_ref[x, :, columns(j)] + own, j)
    sums = [rr_ref[:8]] + [jnp.zeros((8, LANES), F32)] * 2

    def emit(at, w):
        w_ref[at] = w
        sums[1] = sums[1] + rows_sum(r_ref[at] * w)
        sums[2] = sums[2] + rows_sum(w * w)

    for x in range(layers):
        for first in range(0, ny, CHUNK):
            stencil(z_ref, sigma_ref, wind_ref, x, first, CHUNK, emit)
        local2_ref[x] = dot3(halves(w_ref[x]), (high_ref[...], low_ref[...]))
    summed = w_ref[0]
    for x in range(1, layers):
        summed = summed + w_ref[x]
    packed = project(summed, by_ref[...], bz_ref[...], fold)
    send_proj(packed, [jnp.sum(s, axis=0, keepdims=True) for s in sums], pair2_ref, ny)
    send_edges(local2_ref, pair2_ref, odd2_ref)


def lane_of(row, which):
    lane = lax.broadcasted_iota(jnp.int32, row.shape, 1)
    return full_sum(jnp.where(lane == which, row, 0.0))


def first_scalars(gath_ref, rows):
    size = rows // 2 + 1
    row = gath_ref[size - 1 : size]
    for i in range(2, gath_ref.shape[0] // size, 2):
        row = row + gath_ref[(i + 1) * size - 1 : (i + 1) * size]
    rr, rw, ww = (lane_of(row, i) for i in range(3))
    inv_rr = 1.0 / rr
    beta = jnp.sqrt(rr)
    h11 = rw * inv_rr
    h21 = jnp.sqrt(ww * inv_rr - h11 * h11)
    return beta, h11, h21


def last_kernel(
    gath_ref, spread_ref, local_ref, even_ref, odd_ref, r_ref, z_ref, w_ref,
    sigma_ref, wind_ref, z2_ref, u_ref, out_ref, known_ref, *, rows,
):
    layers, ny, _ = r_ref.shape
    beta, h11, h21 = first_scalars(gath_ref, rows)
    scale = 1.0 / (h21 * beta)
    minus = scale * h11
    clear_pads(z2_ref)

    def combine(index, image, j):
        old = z_ref[index, j, PAD : PAD + ny]
        fill_tiles(z2_ref, index, scale * image - minus * old, j)

    for j in range(tiles_of(r_ref)):
        before, after = halo_of(even_ref, odd_ref, j)
        combine(0, spread_ref[0, :, columns(j)] + before, j)
        combine(layers + 1, spread_ref[2, :, columns(j)] + after, j)
        own = spread_ref[1, :, columns(j)]
        for x in range(layers):
            combine(x + 1, local_ref[x, :, columns(j)] + own, j)
    sums = [jnp.zeros((8, LANES), F32)] * 3

    def emit(at, u):
        u_ref[at] = u
        for i, product in enumerate((r_ref[at] * u, w_ref[at] * u, u * u)):
            sums[i] = sums[i] + rows_sum(product)

    for x in range(layers):
        for first in range(0, ny, CHUNK):
            stencil(z2_ref, sigma_ref, wind_ref, x, first, CHUNK, emit)
    lane = lax.broadcasted_iota(jnp.int32, (1, LANES), 1)
    a, b, c = (full_sum(s) for s in sums)
    b = scale * b - minus * a
    row = jnp.where(lane == 0, a, jnp.where(lane == 1, b, jnp.where(lane == 2, c, 0.0)))
    out_ref[...] = jnp.broadcast_to(row, out_ref.shape)
    for i, value in enumerate((beta, h11, h21)):
        known_ref[8 * i : 8 * i + 8] = jnp.broadcast_to(value, (8, LANES))


def finish_kernel(
    sums_ref, known_ref, r_ref, z_ref, w_ref, z2_ref, u_ref, sol_hbm, res_hbm,
    sol_ref, res_ref, sems,
):
    layers, ny, _ = r_ref.shape
    beta, h11, h21 = (known_ref[8 * i : 8 * i + 1, :1] for i in range(3))
    sums = jnp.sum(sums_ref[...], axis=0, keepdims=True)
    h12 = lane_of(sums, 0) / beta
    h22 = lane_of(sums, 1)
    h32 = jnp.sqrt(lane_of(sums, 2) - h12 * h12 - h22 * h22)
    m11 = h11 * h11 + h21 * h21
    m12 = h11 * h12 + h21 * h22
    m22 = h12 * h12 + h22 * h22 + h32 * h32
    q_one = h11 * beta
    q_two = h12 * beta
    determ = m11 * m22 - m12 * m12
    y_one = (m22 * q_one - m12 * q_two) / determ / beta
    y_two = (m11 * q_two - m12 * q_one) / determ
    stores = []
    for x in range(layers):
        for j in range(tiles_of(r_ref)):
            inside = (x + 1, j, slice(PAD, PAD + ny))
            sol_ref[x, :, columns(j)] = y_one * z_ref[inside] + y_two * z2_ref[inside]
        res_ref[x] = r_ref[x] - (y_one * w_ref[x] + y_two * u_ref[x])
        for i, (src, dst) in enumerate(((sol_ref, sol_hbm), (res_ref, res_hbm))):
            store = pltpu.make_async_copy(src.at[x], dst.at[x], sems.at[2 * x + i])
            store.start()
            stores.append(store)
    for store in stores:
        store.wait()


def call(kernel, outs, args, scratch=(), flops=0, hbm=(), far_out=False, limit=24):
    vmem = pl.BlockSpec(memory_space=pltpu.VMEM)
    far = pl.BlockSpec(memory_space=pltpu.HBM)
    outs = [s if isinstance(s, jax.ShapeDtypeStruct) else jax.ShapeDtypeStruct(s, F32) for s in outs]
    return pl.pallas_call(
        kernel,
        out_shape=outs,
        in_specs=[far if i in hbm else vmem for i in range(len(args))],
        out_specs=[far if far_out else vmem] * len(outs),
        scratch_shapes=[pltpu.VMEM(s, F32) if isinstance(s, tuple) else s for s in scratch],
        compiler_params=pltpu.CompilerParams(vmem_limit_bytes=limit << 20),
        cost_estimate=pl.CostEstimate(flops=flops, bytes_accessed=0, transcendentals=0),
    )(*args)


def exchange(block):
    return lax.all_to_all(block, AXIS, 0, 0, tiled=True)


def on_device(right_side, sigma, wind, local_inverse, basis_y, basis_z, gamma):
    count = lax.axis_size(AXIS)
    levels = count.bit_length() - 1
    layers, ny, nz = right_side.shape
    ky, kz = basis_y.shape[1], basis_z.shape[1]
    fold = fold_of(ky, kz)
    rows, width = ky // fold, kz * fold
    field = (layers, ny, nz)
    edge = (1, ny, nz)
    pairs = [(i, i ^ 1) for i in range(count)]
    others = [(i, i + 1) for i in range(1, count - 1, 2)]
    others = others + [(j, i) for i, j in others]
    matmul = 6 * layers * ny * nz * nz
    by, bz = basis_y.T, basis_z.T
    each = rows // 2
    pair = (ny + each, nz)
    tiled = (layers + 2, nz // LANES, ny + 2 * PAD, LANES)

    def round_of(sent, odd, extra):
        got = lax.ppermute(sent, AXIS, pairs)
        odd = lax.ppermute(odd, AXIS, others)
        size = each + extra
        (block,) = call(
            functools.partial(join_kernel, rows=rows, width=width, extra=extra),
            [(count * size, width)], (got, sent), flops=matmul // 16,
        )
        block = exchange(block.reshape(count * size, 1, width)).reshape(count * size, width)
        (spread,) = call(
            functools.partial(
                coarse_kernel, fold=fold, levels=levels, count=count, rows=rows, layers=layers
            ),
            [(3, ny, nz)], (block, by, bz, gamma), [(count, rows, width)],
            flops=matmul // 8,
        )
        return block, spread, got, odd

    square = jax.ShapeDtypeStruct((nz, nz), BF16)
    local, summed, odd, high, low, rr = call(
        first_kernel, [field, (ny, nz), edge, square, square, (32, LANES)],
        (right_side, local_inverse),
        [field, (nz, nz), pltpu.SemaphoreType.DMA((layers + 1,))],
        flops=matmul, hbm=(0, 1), limit=FIRST_LIMIT,
    )
    (sent,) = call(
        functools.partial(project_kernel, fold=fold), [pair],
        (summed, local, by, bz), flops=matmul // 8,
    )
    _, spread, got, odd = round_of(sent, odd, 0)
    z, w, sent, local, odd = call(
        functools.partial(middle_kernel, fold=fold),
        [tiled, field, pair, field, edge],
        (spread, local, got, odd, right_side, sigma, wind, by, bz, high, low, rr),
        flops=2 * matmul,
    )
    gathered, spread, got, odd = round_of(sent, odd, 1)
    z2, u, sent, known = call(
        functools.partial(last_kernel, rows=rows),
        [tiled, field, (count, LANES), (32, LANES)],
        (gathered, spread, local, got, odd, right_side, z, w, sigma, wind), flops=matmul,
    )
    sums = exchange(sent)
    return call(
        finish_kernel, [field, field], (sums, known, right_side, z, w, z2, u),
        [field, field, pltpu.SemaphoreType.DMA((2 * layers,))],
        flops=matmul // 8, far_out=True,
    )


def solution(mesh):
    placed = (P(AXIS, None, None),) * 4 + (P(),) * 3
    return jax.shard_map(
        lambda *args: tuple(on_device(*args)),
        mesh=mesh,
        in_specs=placed,
        out_specs=(P(AXIS, None, None), P(AXIS, None, None)),
        check_vma=False,
    )
```

```python
import functools
import jax
import jax.numpy as jnp
from jax import lax
from jax.experimental import pallas as pl
from jax.experimental.pallas import tpu as pltpu
from jax.sharding import PartitionSpec as P


F32 = jnp.float32
BF16 = jnp.bfloat16
AXIS = "sub"
LANES = 128
NN = (((1,), (0,)), ((), ()))
NT = (((1,), (1,)), ((), ()))
TN = (((0,), (0,)), ((), ()))
CHUNK = 16
FIRST_LIMIT = 51


def halves(x):
    high = x.astype(BF16)
    return high, (x - high.astype(F32)).astype(BF16)


def dot3(left, right, dims=NN):
    lh, ll = left
    rh, rl = right
    mul = functools.partial(lax.dot_general, dimension_numbers=dims, preferred_element_type=F32)
    return mul(lh, rh) + (mul(lh, rl) + mul(ll, rh))


def fold_of(ky, kz):
    fold = max(1, LANES // kz)
    while ky % fold:
        fold //= 2
    return fold


def pack(block, fold):
    rows = block.shape[0] // fold
    return jnp.concatenate([block[i * rows : (i + 1) * rows] for i in range(fold)], axis=1)


def unpack(block, fold):
    cols = block.shape[1] // fold
    return jnp.concatenate([block[:, i * cols : (i + 1) * cols] for i in range(fold)], axis=0)


def project(summed, by, bz, fold):
    half = dot3(halves(summed), halves(bz), NT)
    return pack(dot3(halves(by), halves(half)), fold)


def join_kernel(got_ref, own_ref, out_ref, *, rows, width, extra):
    each = rows // 2
    first = got_ref.shape[0] - each
    both = got_ref[first:] + own_ref[first:]
    half = jnp.where(even_here(), both[:, :width], both[:, width : 2 * width])
    if not extra:
        for i in range(out_ref.shape[0] // each):
            out_ref[i * each : (i + 1) * each] = half
        return
    sums = [full_sum(both[i : i + 1, 2 * width : 2 * width + LANES]) for i in range(3)]
    lane = lax.broadcasted_iota(jnp.int32, (1, width), 1)
    row = jnp.where(
        lane == 0, sums[0], jnp.where(lane == 1, sums[1], jnp.where(lane == 2, sums[2], 0.0))
    )
    block = jnp.concatenate([half, row], axis=0)
    size = each + 1
    for i in range(out_ref.shape[0] // size):
        out_ref[i * size : (i + 1) * size] = block


def coarse_kernel(
    gath_ref, gamma_ref, out_ref, tree_ref, *, fold, levels, count, rows, layers
):
    each = rows // 2
    stride = gath_ref.shape[0] // count
    for i in range(count):
        tree_ref[i // 2, (i % 2) * each : (i % 2 + 1) * each] = gath_ref[
            i * stride : i * stride + each
        ]
    offsets = [0]
    for level in range(1, levels):
        base, size = offsets[-1] + (count >> level), count >> (level + 1)
        pairs = tree_ref[offsets[-1] : base].reshape((size, 2) + tree_ref.shape[1:])
        tree_ref[base : base + size] = pairs[:, 0] + pairs[:, 1]
        offsets.append(base)
    scaled = [
        pack(gamma_ref[level], fold) * (1.0 / (layers * 2.0 ** (level + 1)) ** 0.5)
        for level in range(levels)
    ]
    me = lax.axis_index(AXIS)
    coarse = []
    for shift in (-1, 0, 1):
        who = jnp.clip(me + shift, 0, count - 1)
        total = scaled[0] * tree_ref[offsets[0] + (who >> 1)]
        for level in range(1, levels):
            total = total + scaled[level] * tree_ref[offsets[level] + (who >> (level + 1))]
        if shift:
            total = total * (me + shift == who).astype(F32)
        coarse.append(unpack(total, fold))
    for i, block in enumerate(coarse):
        out_ref[i * block.shape[0] : (i + 1) * block.shape[0], : block.shape[1]] = block


def fill_spreads(coarse_ref, by_ref, bz_ref, spread_ref):
    ky = by_ref.shape[0]
    back_high, back_low = halves(
        dot3(halves(coarse_ref[: 3 * ky, : bz_ref.shape[0]]), halves(bz_ref[...]))
    )
    by_high, by_low = halves(by_ref[...])
    left = jnp.concatenate([by_high, by_high, by_low], axis=0)
    for i in range(spread_ref.shape[0]):
        high, low = (part[i * ky : (i + 1) * ky] for part in (back_high, back_low))
        right = jnp.concatenate([high, low, high], axis=0)
        spread_ref[i] = lax.dot_general(left, right, TN, preferred_element_type=F32)


PAD = 8


def tiles_of(ref):
    return ref.shape[-1] // LANES


def columns(j):
    return slice(j * LANES, (j + 1) * LANES)


def fill_tiles(tiled_ref, index, tile, j):
    ny = tile.shape[0]
    tiled_ref[index, j, PAD : PAD + ny] = tile


def clear_pads(tiled_ref):
    layers, tiles, full, _ = tiled_ref.shape
    zero = jnp.zeros((PAD, LANES), F32)
    for x in range(1, layers - 1):
        for j in range(tiles):
            tiled_ref[x, j, :PAD] = zero
            tiled_ref[x, j, full - PAD :] = zero


def stencil(tiled_ref, sigma_ref, wind_ref, x, first, rows, emit):
    tiles = tiled_ref.shape[1]
    lane = lax.broadcasted_iota(jnp.int32, (rows, LANES), 1)
    top = PAD + first
    here = [tiled_ref[x + 1, j, top : top + rows] for j in range(tiles)]
    up = [pltpu.roll(h, LANES - 1, 1) for h in here] + [jnp.zeros_like(here[0])]
    down = [jnp.zeros_like(here[0])] + [pltpu.roll(h, 1, 1) for h in here]
    for j in range(tiles):
        prev = tiled_ref[x, j, top : top + rows]
        after = tiled_ref[x + 2, j, top : top + rows]
        beside = (
            (after + prev)
            + (tiled_ref[x + 1, j, top - 1 : top - 1 + rows] + tiled_ref[x + 1, j, top + 1 : top + 1 + rows])
            + (
                jnp.where(lane == LANES - 1, up[j + 1], up[j])
                + jnp.where(lane == 0, down[j], down[j + 1])
            )
        )
        at = (x, slice(first, first + rows), columns(j))
        value = (6.0 + sigma_ref[at]) * here[j] - beside + wind_ref[at] * (after - prev)
        emit(at, value)


def rows_sum(x):
    return jnp.sum(x.reshape(x.shape[0] // 8, 8, LANES), axis=0)


def full_sum(x):
    return jnp.sum(x, axis=(0, 1), keepdims=True)


def even_here():
    return lax.rem(lax.axis_index(AXIS), 2) == 0


def send_edges(local_ref, pair_ref, odd_ref):
    layers, ny, _ = local_ref.shape
    even = even_here()
    pair_ref[:ny] = local_ref[jnp.where(even, layers - 1, 0)]
    odd_ref[0] = local_ref[jnp.where(even, 0, layers - 1)]


def send_proj(packed, scalars, pair_ref, ny):
    each = packed.shape[0] // 2
    parts = [packed[:each], packed[each:]]
    if scalars:
        parts.append(jnp.concatenate(scalars + [jnp.zeros((each - len(scalars), LANES), F32)], axis=0))
    used = sum(p.shape[1] for p in parts)
    if used < pair_ref.shape[1]:
        parts.append(jnp.zeros((each, pair_ref.shape[1] - used), F32))
    pair_ref[ny:] = jnp.concatenate(parts, axis=1)


def first_kernel(
    r_hbm, inv_hbm, local_ref, summed_ref, odd_ref, high_ref, low_ref, rr_ref, r_ref, inv_ref, sems
):
    layers, _, nz = r_ref.shape
    half = nz // 2
    moves = [(inv_hbm.at[0, :half], inv_ref.at[:half])]
    moves += [(r_hbm.at[x], r_ref.at[x]) for x in range(layers)]
    moves += [(inv_hbm.at[0, half:], inv_ref.at[half:])]
    loads = [pltpu.make_async_copy(*move, sems.at[i]) for i, move in enumerate(moves)]
    for load in loads:
        load.start()
    loads[0].wait()
    upper = halves(inv_ref[:half])
    high_ref[:half], low_ref[:half] = upper
    total = jnp.zeros((8, LANES), F32)
    for x in range(layers):
        loads[x + 1].wait()
        local_ref[x] = dot3(halves(r_ref[x, :, :half]), upper)
        for j in range(tiles_of(r_ref)):
            r = r_ref[x, :, columns(j)]
            total = total + rows_sum(r * r)
            summed_ref[:, columns(j)] = r if x == 0 else summed_ref[:, columns(j)] + r
    rr_ref[:8] = total
    loads[layers + 1].wait()
    lower = halves(inv_ref[half:])
    high_ref[half:], low_ref[half:] = lower
    for x in range(layers):
        local_ref[x] += dot3(halves(r_ref[x, :, half:]), lower)
    odd_ref[0] = local_ref[jnp.where(even_here(), 0, layers - 1)]


def project_kernel(summed_ref, local_ref, by_ref, bz_ref, pair_ref, *, fold):
    layers, ny, _ = local_ref.shape
    pair_ref[:ny] = local_ref[jnp.where(even_here(), layers - 1, 0)]
    send_proj(project(summed_ref[...], by_ref[...], bz_ref[...], fold), [], pair_ref, ny)


def halo_of(even_ref, odd_ref, j):
    ny = odd_ref.shape[1]
    even = even_here()
    pair = even_ref[:ny, columns(j)]
    odd = odd_ref[0, :, columns(j)]
    return jnp.where(even, odd, pair), jnp.where(even, pair, odd)


def middle_kernel(
    coarse_ref, local_ref, even_ref, odd_ref, r_ref, sigma_ref, wind_ref, by_ref, bz_ref,
    high_ref, low_ref, rr_ref,
    z_ref, w_ref, pair2_ref, local2_ref, odd2_ref, spread_ref, *, fold,
):
    layers, ny, _ = r_ref.shape
    fill_spreads(coarse_ref, by_ref, bz_ref, spread_ref)
    clear_pads(z_ref)
    for j in range(tiles_of(r_ref)):
        before, after = halo_of(even_ref, odd_ref, j)
        fill_tiles(z_ref, 0, spread_ref[0, :, columns(j)] + before, j)
        fill_tiles(z_ref, layers + 1, spread_ref[2, :, columns(j)] + after, j)
        own = spread_ref[1, :, columns(j)]
        for x in range(layers):
            fill_tiles(z_ref, x + 1, local_ref[x, :, columns(j)] + own, j)
    sums = [rr_ref[:8]] + [jnp.zeros((8, LANES), F32)] * 2

    def emit(at, w):
        w_ref[at] = w
        sums[1] = sums[1] + rows_sum(r_ref[at] * w)
        sums[2] = sums[2] + rows_sum(w * w)

    for x in range(layers):
        for first in range(0, ny, CHUNK):
            stencil(z_ref, sigma_ref, wind_ref, x, first, CHUNK, emit)
        if x % 2:
            both = halves(w_ref[x - 1 : x + 1].reshape(2 * ny, -1))
            product = dot3(both, (high_ref[...], low_ref[...]))
            local2_ref[x - 1 : x + 1] = product.reshape(2, ny, -1)
    summed = w_ref[0]
    for x in range(1, layers):
        summed = summed + w_ref[x]
    packed = project(summed, by_ref[...], bz_ref[...], fold)
    send_proj(packed, [jnp.sum(s, axis=0, keepdims=True) for s in sums], pair2_ref, ny)
    send_edges(local2_ref, pair2_ref, odd2_ref)


def lane_of(row, which):
    lane = lax.broadcasted_iota(jnp.int32, row.shape, 1)
    return full_sum(jnp.where(lane == which, row, 0.0))


def first_scalars(gath_ref, rows):
    size = rows // 2 + 1
    row = gath_ref[size - 1 : size]
    for i in range(2, gath_ref.shape[0] // size, 2):
        row = row + gath_ref[(i + 1) * size - 1 : (i + 1) * size]
    rr, rw, ww = (lane_of(row, i) for i in range(3))
    inv_rr = 1.0 / rr
    beta = jnp.sqrt(rr)
    h11 = rw * inv_rr
    h21 = jnp.sqrt(ww * inv_rr - h11 * h11)
    return beta, h11, h21


def last_kernel(
    gath_ref, coarse_ref, local_ref, even_ref, odd_ref, r_ref, z_ref, w_ref,
    sigma_ref, wind_ref, by_ref, bz_ref, z2_ref, u_ref, out_ref, known_ref, spread_ref, *, rows,
):
    layers, ny, _ = r_ref.shape
    fill_spreads(coarse_ref, by_ref, bz_ref, spread_ref)
    beta, h11, h21 = first_scalars(gath_ref, rows)
    scale = 1.0 / (h21 * beta)
    minus = scale * h11
    clear_pads(z2_ref)

    def combine(index, image, j):
        old = z_ref[index, j, PAD : PAD + ny]
        fill_tiles(z2_ref, index, scale * image - minus * old, j)

    for j in range(tiles_of(r_ref)):
        before, after = halo_of(even_ref, odd_ref, j)
        combine(0, spread_ref[0, :, columns(j)] + before, j)
        combine(layers + 1, spread_ref[2, :, columns(j)] + after, j)
        own = spread_ref[1, :, columns(j)]
        for x in range(layers):
            combine(x + 1, local_ref[x, :, columns(j)] + own, j)
    sums = [jnp.zeros((8, LANES), F32)] * 3

    def emit(at, u):
        u_ref[at] = u
        for i, product in enumerate((r_ref[at] * u, w_ref[at] * u, u * u)):
            sums[i] = sums[i] + rows_sum(product)

    for x in range(layers):
        for first in range(0, ny, CHUNK):
            stencil(z2_ref, sigma_ref, wind_ref, x, first, CHUNK, emit)
    lane = lax.broadcasted_iota(jnp.int32, (1, LANES), 1)
    a, b, c = (full_sum(s) for s in sums)
    b = scale * b - minus * a
    row = jnp.where(lane == 0, a, jnp.where(lane == 1, b, jnp.where(lane == 2, c, 0.0)))
    out_ref[...] = jnp.broadcast_to(row, out_ref.shape)
    for i, value in enumerate((beta, h11, h21)):
        known_ref[8 * i : 8 * i + 8] = jnp.broadcast_to(value, (8, LANES))


def finish_kernel(
    sums_ref, known_ref, r_ref, z_ref, w_ref, z2_ref, u_ref, sol_hbm, res_hbm,
    sol_ref, res_ref, sems,
):
    layers, ny, _ = r_ref.shape
    beta, h11, h21 = (known_ref[8 * i : 8 * i + 1, :1] for i in range(3))
    sums = jnp.sum(sums_ref[...], axis=0, keepdims=True)
    h12 = lane_of(sums, 0) / beta
    h22 = lane_of(sums, 1)
    h32 = jnp.sqrt(lane_of(sums, 2) - h12 * h12 - h22 * h22)
    m11 = h11 * h11 + h21 * h21
    m12 = h11 * h12 + h21 * h22
    m22 = h12 * h12 + h22 * h22 + h32 * h32
    q_one = h11 * beta
    q_two = h12 * beta
    determ = m11 * m22 - m12 * m12
    y_one = (m22 * q_one - m12 * q_two) / determ / beta
    y_two = (m11 * q_two - m12 * q_one) / determ
    stores = []
    for x in range(layers):
        for j in range(tiles_of(r_ref)):
            inside = (x + 1, j, slice(PAD, PAD + ny))
            sol_ref[x, :, columns(j)] = y_one * z_ref[inside] + y_two * z2_ref[inside]
        res_ref[x] = r_ref[x] - (y_one * w_ref[x] + y_two * u_ref[x])
        for i, (src, dst) in enumerate(((sol_ref, sol_hbm), (res_ref, res_hbm))):
            store = pltpu.make_async_copy(src.at[x], dst.at[x], sems.at[2 * x + i])
            store.start()
            stores.append(store)
    for store in stores:
        store.wait()


def call(kernel, outs, args, scratch=(), flops=0, hbm=(), far_out=False, limit=24):
    vmem = pl.BlockSpec(memory_space=pltpu.VMEM)
    far = pl.BlockSpec(memory_space=pltpu.HBM)
    outs = [s if isinstance(s, jax.ShapeDtypeStruct) else jax.ShapeDtypeStruct(s, F32) for s in outs]
    return pl.pallas_call(
        kernel,
        out_shape=outs,
        in_specs=[far if i in hbm else vmem for i in range(len(args))],
        out_specs=[far if far_out else vmem] * len(outs),
        scratch_shapes=[pltpu.VMEM(s, F32) if isinstance(s, tuple) else s for s in scratch],
        compiler_params=pltpu.CompilerParams(vmem_limit_bytes=limit << 20),
        cost_estimate=pl.CostEstimate(flops=flops, bytes_accessed=0, transcendentals=0),
    )(*args)


def exchange(block):
    return lax.all_to_all(block, AXIS, 0, 0, tiled=True)


def on_device(right_side, sigma, wind, local_inverse, basis_y, basis_z, gamma):
    count = lax.axis_size(AXIS)
    levels = count.bit_length() - 1
    layers, ny, nz = right_side.shape
    ky, kz = basis_y.shape[1], basis_z.shape[1]
    fold = fold_of(ky, kz)
    rows, width = ky // fold, kz * fold
    field = (layers, ny, nz)
    edge = (1, ny, nz)
    pairs = [(i, i ^ 1) for i in range(count)]
    others = [(i, i + 1) for i in range(1, count - 1, 2)]
    others = others + [(j, i) for i, j in others]
    matmul = 6 * layers * ny * nz * nz
    by, bz = basis_y.T, basis_z.T
    each = rows // 2
    pair = (ny + each, nz)
    tiled = (layers + 2, nz // LANES, ny + 2 * PAD, LANES)

    def round_of(sent, odd, extra):
        got = lax.ppermute(sent, AXIS, pairs)
        odd = lax.ppermute(odd, AXIS, others)
        size = each + extra
        (block,) = call(
            functools.partial(join_kernel, rows=rows, width=width, extra=extra),
            [(count * size, width)], (got, sent), flops=matmul // 16,
        )
        block = exchange(block.reshape(count * size, 1, width)).reshape(count * size, width)
        (coarse,) = call(
            functools.partial(
                coarse_kernel, fold=fold, levels=levels, count=count, rows=rows, layers=layers
            ),
            [(-(-3 * ky // 32) * 32, LANES)], (block, gamma), [(count, rows, width)],
            flops=matmul // 16,
        )
        return block, coarse, got, odd

    square = jax.ShapeDtypeStruct((nz, nz), BF16)
    local, summed, odd, high, low, rr = call(
        first_kernel, [field, (ny, nz), edge, square, square, (32, LANES)],
        (right_side, local_inverse),
        [field, (nz, nz), pltpu.SemaphoreType.DMA((layers + 2,))],
        flops=matmul, hbm=(0, 1), limit=FIRST_LIMIT,
    )
    (sent,) = call(
        functools.partial(project_kernel, fold=fold), [pair],
        (summed, local, by, bz), flops=matmul // 8,
    )
    _, coarse, got, odd = round_of(sent, odd, 0)
    z, w, sent, local, odd = call(
        functools.partial(middle_kernel, fold=fold),
        [tiled, field, pair, field, edge],
        (coarse, local, got, odd, right_side, sigma, wind, by, bz, high, low, rr),
        [(3, ny, nz)], flops=2 * matmul,
    )
    gathered, coarse, got, odd = round_of(sent, odd, 1)
    z2, u, sent, known = call(
        functools.partial(last_kernel, rows=rows),
        [tiled, field, (count, LANES), (32, LANES)],
        (gathered, coarse, local, got, odd, right_side, z, w, sigma, wind, by, bz),
        [(3, ny, nz)], flops=matmul,
    )
    sums = exchange(sent)
    return call(
        finish_kernel, [field, field], (sums, known, right_side, z, w, z2, u),
        [field, field, pltpu.SemaphoreType.DMA((2 * layers,))],
        flops=matmul // 8, far_out=True,
    )


def solution(mesh):
    placed = (P(AXIS, None, None),) * 4 + (P(),) * 3
    return jax.shard_map(
        lambda *args: tuple(on_device(*args)),
        mesh=mesh,
        in_specs=placed,
        out_specs=(P(AXIS, None, None), P(AXIS, None, None)),
        check_vma=False,
    )
```

```python
import functools
import jax
import jax.numpy as jnp
from jax import lax
from jax.experimental import pallas as pl
from jax.experimental.pallas import tpu as pltpu
from jax.sharding import PartitionSpec as P


F32 = jnp.float32
BF16 = jnp.bfloat16
AXIS = "sub"
LANES = 128
NN = (((1,), (0,)), ((), ()))
NT = (((1,), (1,)), ((), ()))
TN = (((0,), (0,)), ((), ()))
CHUNK = 16
FIRST_LIMIT = 50


def halves(x):
    high = x.astype(BF16)
    return high, (x - high.astype(F32)).astype(BF16)


def dot3(left, right, dims=NN):
    lh, ll = left
    rh, rl = right
    mul = functools.partial(lax.dot_general, dimension_numbers=dims, preferred_element_type=F32)
    return mul(lh, rh) + (mul(lh, rl) + mul(ll, rh))


def fold_of(ky, kz):
    fold = max(1, LANES // kz)
    while ky % fold:
        fold //= 2
    return fold


def pack(block, fold):
    rows = block.shape[0] // fold
    return jnp.concatenate([block[i * rows : (i + 1) * rows] for i in range(fold)], axis=1)


def unpack(block, fold):
    cols = block.shape[1] // fold
    return jnp.concatenate([block[:, i * cols : (i + 1) * cols] for i in range(fold)], axis=0)


def project(summed, by, bz, fold):
    high, low = halves(summed)
    by_high, by_low = halves(by)
    half = lax.dot_general(
        jnp.concatenate([by_high, by_low], axis=0), high, NN, preferred_element_type=F32
    )
    ky = by.shape[0]
    half = half[:ky] + (half[ky:] + jnp.dot(by_high, low, preferred_element_type=F32))
    return pack(dot3(halves(half), halves(bz), NT), fold)


def join_kernel(got_ref, own_ref, out_ref, *, rows, width, extra):
    each = rows // 2
    first = got_ref.shape[0] - each
    both = got_ref[first:] + own_ref[first:]
    half = jnp.where(even_here(), both[:, :width], both[:, width : 2 * width])
    if not extra:
        for i in range(out_ref.shape[0] // each):
            out_ref[i * each : (i + 1) * each] = half
        return
    sums = [full_sum(both[i : i + 1, 2 * width : 2 * width + LANES]) for i in range(3)]
    lane = lax.broadcasted_iota(jnp.int32, (1, width), 1)
    row = jnp.where(
        lane == 0, sums[0], jnp.where(lane == 1, sums[1], jnp.where(lane == 2, sums[2], 0.0))
    )
    block = jnp.concatenate([half, row], axis=0)
    size = each + 1
    for i in range(out_ref.shape[0] // size):
        out_ref[i * size : (i + 1) * size] = block


def coarse_kernel(
    gath_ref, gamma_ref, out_ref, tree_ref, *, fold, levels, count, rows, layers
):
    each = rows // 2
    stride = gath_ref.shape[0] // count
    for i in range(count):
        tree_ref[i // 2, (i % 2) * each : (i % 2 + 1) * each] = gath_ref[
            i * stride : i * stride + each
        ]
    offsets = [0]
    for level in range(1, levels):
        base, size = offsets[-1] + (count >> level), count >> (level + 1)
        pairs = tree_ref[offsets[-1] : base].reshape((size, 2) + tree_ref.shape[1:])
        tree_ref[base : base + size] = pairs[:, 0] + pairs[:, 1]
        offsets.append(base)
    scaled = [
        pack(gamma_ref[level], fold) * (1.0 / (layers * 2.0 ** (level + 1)) ** 0.5)
        for level in range(levels)
    ]
    me = lax.axis_index(AXIS)
    coarse = []
    for shift in (-1, 0, 1):
        who = jnp.clip(me + shift, 0, count - 1)
        total = scaled[0] * tree_ref[offsets[0] + (who >> 1)]
        for level in range(1, levels):
            total = total + scaled[level] * tree_ref[offsets[level] + (who >> (level + 1))]
        if shift:
            total = total * (me + shift == who).astype(F32)
        coarse.append(unpack(total, fold))
    for i, block in enumerate(coarse):
        out_ref[i * block.shape[0] : (i + 1) * block.shape[0], : block.shape[1]] = block


def fill_spreads(coarse_ref, by_ref, bz_ref, spread_ref):
    ky = by_ref.shape[0]
    back_high, back_low = halves(
        dot3(halves(coarse_ref[: 3 * ky, : bz_ref.shape[0]]), halves(bz_ref[...]))
    )
    by_high, by_low = halves(by_ref[...])
    left = jnp.concatenate([by_high, by_high, by_low], axis=0)
    for i in range(spread_ref.shape[0]):
        high, low = (part[i * ky : (i + 1) * ky] for part in (back_high, back_low))
        right = jnp.concatenate([high, low, high], axis=0)
        spread_ref[i] = lax.dot_general(left, right, TN, preferred_element_type=F32)


PAD = 8


def tiles_of(ref):
    return ref.shape[-1] // LANES


def columns(j):
    return slice(j * LANES, (j + 1) * LANES)


def fill_tiles(tiled_ref, index, tile, j):
    ny = tile.shape[0]
    tiled_ref[index, j, PAD : PAD + ny] = tile


def clear_pads(tiled_ref):
    layers, tiles, full, _ = tiled_ref.shape
    zero = jnp.zeros((PAD, LANES), F32)
    for x in range(1, layers - 1):
        for j in range(tiles):
            tiled_ref[x, j, :PAD] = zero
            tiled_ref[x, j, full - PAD :] = zero


def stencil(tiled_ref, sigma_ref, wind_ref, x, first, rows, emit):
    tiles = tiled_ref.shape[1]
    lane = lax.broadcasted_iota(jnp.int32, (rows, LANES), 1)
    top = PAD + first
    here = [tiled_ref[x + 1, j, top : top + rows] for j in range(tiles)]
    up = [pltpu.roll(h, LANES - 1, 1) for h in here] + [jnp.zeros_like(here[0])]
    down = [jnp.zeros_like(here[0])] + [pltpu.roll(h, 1, 1) for h in here]
    for j in range(tiles):
        prev = tiled_ref[x, j, top : top + rows]
        after = tiled_ref[x + 2, j, top : top + rows]
        beside = (
            (after + prev)
            + (tiled_ref[x + 1, j, top - 1 : top - 1 + rows] + tiled_ref[x + 1, j, top + 1 : top + 1 + rows])
            + (
                jnp.where(lane == LANES - 1, up[j + 1], up[j])
                + jnp.where(lane == 0, down[j], down[j + 1])
            )
        )
        at = (x, slice(first, first + rows), columns(j))
        value = (6.0 + sigma_ref[at]) * here[j] - beside + wind_ref[at] * (after - prev)
        emit(at, value)


def rows_sum(x):
    return jnp.sum(x.reshape(x.shape[0] // 8, 8, LANES), axis=0)


def full_sum(x):
    return jnp.sum(x, axis=(0, 1), keepdims=True)


def even_here():
    return lax.rem(lax.axis_index(AXIS), 2) == 0


def send_edges(local_ref, pair_ref, odd_ref):
    layers, ny, _ = local_ref.shape
    even = even_here()
    pair_ref[:ny] = local_ref[jnp.where(even, layers - 1, 0)]
    odd_ref[0] = local_ref[jnp.where(even, 0, layers - 1)]


def send_proj(packed, scalars, pair_ref, ny):
    each = packed.shape[0] // 2
    parts = [packed[:each], packed[each:]]
    if scalars:
        parts.append(jnp.concatenate(scalars + [jnp.zeros((each - len(scalars), LANES), F32)], axis=0))
    used = sum(p.shape[1] for p in parts)
    if used < pair_ref.shape[1]:
        parts.append(jnp.zeros((each, pair_ref.shape[1] - used), F32))
    pair_ref[ny:] = jnp.concatenate(parts, axis=1)


def first_kernel(
    r_hbm, inv_hbm, local_ref, summed_ref, odd_ref, high_ref, low_ref, rr_ref, r_ref,
    inv_ref, sems
):
    layers, _, nz = r_ref.shape
    half = nz // 2
    moves = [(inv_hbm.at[0, :half], inv_ref.at[:half])]
    moves += [(r_hbm.at[x], r_ref.at[x]) for x in range(layers)]
    moves += [(inv_hbm.at[0, half:], inv_ref.at[half:])]
    loads = [pltpu.make_async_copy(*move, sems.at[i]) for i, move in enumerate(moves)]
    for load in loads:
        load.start()
    loads[0].wait()
    upper = halves(inv_ref[:half])
    high_ref[:half], low_ref[:half] = upper
    total = jnp.zeros((8, LANES), F32)
    for x in range(layers):
        loads[x + 1].wait()
        local_ref[x] = dot3(halves(r_ref[x, :, :half]), upper)
        for j in range(tiles_of(r_ref)):
            r = r_ref[x, :, columns(j)]
            total = total + rows_sum(r * r)
            summed_ref[:, columns(j)] = r if x == 0 else summed_ref[:, columns(j)] + r
    rr_ref[:8] = total
    loads[layers + 1].wait()
    lower = halves(inv_ref[half:])
    high_ref[half:], low_ref[half:] = lower
    for x in range(layers):
        local_ref[x] += dot3(halves(r_ref[x, :, half:]), lower)
    odd_ref[0] = local_ref[jnp.where(even_here(), 0, layers - 1)]


def project_kernel(summed_ref, local_ref, by_ref, bz_ref, pair_ref, *, fold):
    layers, ny, _ = local_ref.shape
    pair_ref[:ny] = local_ref[jnp.where(even_here(), layers - 1, 0)]
    send_proj(project(summed_ref[...], by_ref[...], bz_ref[...], fold), [], pair_ref, ny)


def halo_of(even_ref, odd_ref, j):
    ny = odd_ref.shape[1]
    even = even_here()
    pair = even_ref[:ny, columns(j)]
    odd = odd_ref[0, :, columns(j)]
    return jnp.where(even, odd, pair), jnp.where(even, pair, odd)


def middle_kernel(
    coarse_ref, local_ref, even_ref, odd_ref, r_ref, sigma_ref, wind_ref, by_ref, bz_ref,
    high_ref, low_ref, rr_ref,
    z_ref, w_ref, pair2_ref, local2_ref, odd2_ref, spread_ref, *, fold,
):
    layers, ny, _ = r_ref.shape
    fill_spreads(coarse_ref, by_ref, bz_ref, spread_ref)
    clear_pads(z_ref)
    for j in range(tiles_of(r_ref)):
        before, after = halo_of(even_ref, odd_ref, j)
        fill_tiles(z_ref, 0, spread_ref[0, :, columns(j)] + before, j)
        fill_tiles(z_ref, layers + 1, spread_ref[2, :, columns(j)] + after, j)
        own = spread_ref[1, :, columns(j)]
        for x in range(layers):
            fill_tiles(z_ref, x + 1, local_ref[x, :, columns(j)] + own, j)
    sums = [rr_ref[:8]] + [jnp.zeros((8, LANES), F32)] * 2

    def emit(at, w):
        w_ref[at] = w
        sums[1] = sums[1] + rows_sum(r_ref[at] * w)
        sums[2] = sums[2] + rows_sum(w * w)

    for x in range(layers):
        for first in range(0, ny, CHUNK):
            stencil(z_ref, sigma_ref, wind_ref, x, first, CHUNK, emit)
        if x % 2:
            both = halves(w_ref[x - 1 : x + 1].reshape(2 * ny, -1))
            product = dot3(both, (high_ref[...], low_ref[...]))
            local2_ref[x - 1 : x + 1] = product.reshape(2, ny, -1)
    summed = w_ref[0]
    for x in range(1, layers):
        summed = summed + w_ref[x]
    packed = project(summed, by_ref[...], bz_ref[...], fold)
    send_proj(packed, [jnp.sum(s, axis=0, keepdims=True) for s in sums], pair2_ref, ny)
    send_edges(local2_ref, pair2_ref, odd2_ref)


def lane_of(row, which):
    lane = lax.broadcasted_iota(jnp.int32, row.shape, 1)
    return full_sum(jnp.where(lane == which, row, 0.0))


def first_scalars(gath_ref, rows):
    size = rows // 2 + 1
    row = gath_ref[size - 1 : size]
    for i in range(2, gath_ref.shape[0] // size, 2):
        row = row + gath_ref[(i + 1) * size - 1 : (i + 1) * size]
    rr, rw, ww = (lane_of(row, i) for i in range(3))
    inv_rr = 1.0 / rr
    beta = jnp.sqrt(rr)
    h11 = rw * inv_rr
    h21 = jnp.sqrt(ww * inv_rr - h11 * h11)
    return beta, h11, h21


def last_kernel(
    gath_ref, coarse_ref, local_ref, even_ref, odd_ref, r_ref, z_ref, w_ref,
    sigma_ref, wind_ref, by_ref, bz_ref, z2_ref, u_ref, out_ref, known_ref, spread_ref, *, rows,
):
    layers, ny, _ = r_ref.shape
    fill_spreads(coarse_ref, by_ref, bz_ref, spread_ref)
    beta, h11, h21 = first_scalars(gath_ref, rows)
    scale = 1.0 / (h21 * beta)
    minus = scale * h11
    clear_pads(z2_ref)

    def combine(index, image, j):
        old = z_ref[index, j, PAD : PAD + ny]
        fill_tiles(z2_ref, index, scale * image - minus * old, j)

    for j in range(tiles_of(r_ref)):
        before, after = halo_of(even_ref, odd_ref, j)
        combine(0, spread_ref[0, :, columns(j)] + before, j)
        combine(layers + 1, spread_ref[2, :, columns(j)] + after, j)
        own = spread_ref[1, :, columns(j)]
        for x in range(layers):
            combine(x + 1, local_ref[x, :, columns(j)] + own, j)
    sums = [jnp.zeros((8, LANES), F32)] * 3

    def emit(at, u):
        u_ref[at] = u
        for i, product in enumerate((r_ref[at] * u, w_ref[at] * u, u * u)):
            sums[i] = sums[i] + rows_sum(product)

    for x in range(layers):
        for first in range(0, ny, CHUNK):
            stencil(z2_ref, sigma_ref, wind_ref, x, first, CHUNK, emit)
    lane = lax.broadcasted_iota(jnp.int32, (1, LANES), 1)
    a, b, c = (full_sum(s) for s in sums)
    b = scale * b - minus * a
    row = jnp.where(lane == 0, a, jnp.where(lane == 1, b, jnp.where(lane == 2, c, 0.0)))
    out_ref[...] = jnp.broadcast_to(row, out_ref.shape)
    for i, value in enumerate((beta, h11, h21)):
        known_ref[8 * i : 8 * i + 8] = jnp.broadcast_to(value, (8, LANES))


def finish_kernel(
    sums_ref, known_ref, r_ref, z_ref, w_ref, z2_ref, u_ref, sol_hbm, res_hbm,
    sol_ref, res_ref, sems,
):
    layers, ny, _ = r_ref.shape
    beta, h11, h21 = (known_ref[8 * i : 8 * i + 1, :1] for i in range(3))
    sums = jnp.sum(sums_ref[...], axis=0, keepdims=True)
    h12 = lane_of(sums, 0) / beta
    h22 = lane_of(sums, 1)
    h32 = jnp.sqrt(lane_of(sums, 2) - h12 * h12 - h22 * h22)
    m11 = h11 * h11 + h21 * h21
    m12 = h11 * h12 + h21 * h22
    m22 = h12 * h12 + h22 * h22 + h32 * h32
    q_one = h11 * beta
    q_two = h12 * beta
    determ = m11 * m22 - m12 * m12
    y_one = (m22 * q_one - m12 * q_two) / determ / beta
    y_two = (m11 * q_two - m12 * q_one) / determ
    stores = []
    for x in range(layers):
        for j in range(tiles_of(r_ref)):
            inside = (x + 1, j, slice(PAD, PAD + ny))
            sol_ref[x, :, columns(j)] = y_one * z_ref[inside] + y_two * z2_ref[inside]
        res_ref[x] = r_ref[x] - (y_one * w_ref[x] + y_two * u_ref[x])
        for i, (src, dst) in enumerate(((sol_ref, sol_hbm), (res_ref, res_hbm))):
            store = pltpu.make_async_copy(src.at[x], dst.at[x], sems.at[2 * x + i])
            store.start()
            stores.append(store)
    for store in stores:
        store.wait()


def call(kernel, outs, args, scratch=(), flops=0, hbm=(), far_out=False, limit=24):
    vmem = pl.BlockSpec(memory_space=pltpu.VMEM)
    far = pl.BlockSpec(memory_space=pltpu.HBM)
    outs = [s if isinstance(s, jax.ShapeDtypeStruct) else jax.ShapeDtypeStruct(s, F32) for s in outs]
    return pl.pallas_call(
        kernel,
        out_shape=outs,
        in_specs=[far if i in hbm else vmem for i in range(len(args))],
        out_specs=[far if far_out else vmem] * len(outs),
        scratch_shapes=[pltpu.VMEM(s, F32) if isinstance(s, tuple) else s for s in scratch],
        compiler_params=pltpu.CompilerParams(vmem_limit_bytes=limit << 20),
        cost_estimate=pl.CostEstimate(flops=flops, bytes_accessed=0, transcendentals=0),
    )(*args)


def exchange(block):
    return lax.all_to_all(block, AXIS, 0, 0, tiled=True)


def on_device(right_side, sigma, wind, local_inverse, basis_y, basis_z, gamma):
    count = lax.axis_size(AXIS)
    levels = count.bit_length() - 1
    layers, ny, nz = right_side.shape
    ky, kz = basis_y.shape[1], basis_z.shape[1]
    fold = fold_of(ky, kz)
    rows, width = ky // fold, kz * fold
    field = (layers, ny, nz)
    edge = (1, ny, nz)
    pairs = [(i, i ^ 1) for i in range(count)]
    others = [(i, i + 1) for i in range(1, count - 1, 2)]
    others = others + [(j, i) for i, j in others]
    matmul = 6 * layers * ny * nz * nz
    by, bz = basis_y.T, basis_z.T
    each = rows // 2
    pair = (ny + each, nz)
    tiled = (layers + 2, nz // LANES, ny + 2 * PAD, LANES)

    def round_of(sent, odd, extra):
        got = lax.ppermute(sent, AXIS, pairs)
        odd = lax.ppermute(odd, AXIS, others)
        size = each + extra
        (block,) = call(
            functools.partial(join_kernel, rows=rows, width=width, extra=extra),
            [(count * size, width)], (got, sent), flops=matmul // 16,
        )
        block = exchange(block.reshape(count * size, 1, width)).reshape(count * size, width)
        (coarse,) = call(
            functools.partial(
                coarse_kernel, fold=fold, levels=levels, count=count, rows=rows, layers=layers
            ),
            [(-(-3 * ky // 32) * 32, LANES)], (block, gamma), [(count, rows, width)],
            flops=matmul // 16,
        )
        return block, coarse, got, odd

    square = jax.ShapeDtypeStruct((nz, nz), BF16)
    local, summed, odd, high, low, rr, r = call(
        first_kernel, [field, (ny, nz), edge, square, square, (32, LANES), field],
        (right_side, local_inverse),
        [(nz, nz), pltpu.SemaphoreType.DMA((layers + 2,))],
        flops=matmul, hbm=(0, 1), limit=FIRST_LIMIT,
    )
    (sent,) = call(
        functools.partial(project_kernel, fold=fold), [pair],
        (summed, local, by, bz), flops=matmul // 8,
    )
    _, coarse, got, odd = round_of(sent, odd, 0)
    z, w, sent, local, odd = call(
        functools.partial(middle_kernel, fold=fold),
        [tiled, field, pair, field, edge],
        (coarse, local, got, odd, r, sigma, wind, by, bz, high, low, rr),
        [(3, ny, nz)], flops=2 * matmul,
    )
    gathered, coarse, got, odd = round_of(sent, odd, 1)
    z2, u, sent, known = call(
        functools.partial(last_kernel, rows=rows),
        [tiled, field, (count, LANES), (32, LANES)],
        (gathered, coarse, local, got, odd, r, z, w, sigma, wind, by, bz),
        [(3, ny, nz)], flops=matmul,
    )
    sums = exchange(sent)
    return call(
        finish_kernel, [field, field], (sums, known, r, z, w, z2, u),
        [field, field, pltpu.SemaphoreType.DMA((2 * layers,))],
        flops=matmul // 8, far_out=True,
    )


def solution(mesh):
    placed = (P(AXIS, None, None),) * 4 + (P(),) * 3
    return jax.shard_map(
        lambda *args: tuple(on_device(*args)),
        mesh=mesh,
        in_specs=placed,
        out_specs=(P(AXIS, None, None), P(AXIS, None, None)),
        check_vma=False,
    )
```

```python
import functools
import jax
import jax.numpy as jnp
from jax import lax
from jax.experimental import pallas as pl
from jax.experimental.pallas import tpu as pltpu
from jax.sharding import PartitionSpec as P


F32 = jnp.float32
BF16 = jnp.bfloat16
AXIS = "sub"
LANES = 128
NN = (((1,), (0,)), ((), ()))
NT = (((1,), (1,)), ((), ()))
TN = (((0,), (0,)), ((), ()))
CHUNK = 16
STEP = 2
FIRST_LIMIT = 50


def halves(x):
    high = x.astype(BF16)
    return high, (x - high.astype(F32)).astype(BF16)


def dot3(left, right, dims=NN):
    lh, ll = left
    rh, rl = right
    mul = functools.partial(lax.dot_general, dimension_numbers=dims, preferred_element_type=F32)
    return mul(lh, rh) + (mul(lh, rl) + mul(ll, rh))


def fold_of(ky, kz):
    fold = max(1, LANES // kz)
    while ky % fold:
        fold //= 2
    return fold


def pack(block, fold):
    rows = block.shape[0] // fold
    return jnp.concatenate([block[i * rows : (i + 1) * rows] for i in range(fold)], axis=1)


def unpack(block, fold):
    cols = block.shape[1] // fold
    return jnp.concatenate([block[:, i * cols : (i + 1) * cols] for i in range(fold)], axis=0)


def project(summed, by, bz, fold):
    high, low = halves(summed)
    by_high, by_low = halves(by)
    half = lax.dot_general(
        jnp.concatenate([by_high, by_low], axis=0), high, NN, preferred_element_type=F32
    )
    ky = by.shape[0]
    half = half[:ky] + (half[ky:] + jnp.dot(by_high, low, preferred_element_type=F32))
    return pack(dot3(halves(half), halves(bz), NT), fold)


def join_kernel(got_ref, own_ref, out_ref, *, rows, width, extra):
    each = rows // 2
    first = got_ref.shape[0] - each
    both = got_ref[first:] + own_ref[first:]
    half = jnp.where(even_here(), both[:, :width], both[:, width : 2 * width])
    if not extra:
        for i in range(out_ref.shape[0] // each):
            out_ref[i * each : (i + 1) * each] = half
        return
    sums = [full_sum(both[i : i + 1, 2 * width : 2 * width + LANES]) for i in range(3)]
    lane = lax.broadcasted_iota(jnp.int32, (1, width), 1)
    row = jnp.where(
        lane == 0, sums[0], jnp.where(lane == 1, sums[1], jnp.where(lane == 2, sums[2], 0.0))
    )
    block = jnp.concatenate([half, row], axis=0)
    size = each + 1
    for i in range(out_ref.shape[0] // size):
        out_ref[i * size : (i + 1) * size] = block


def coarse_kernel(
    gath_ref, gamma_ref, out_ref, tree_ref, *, fold, levels, count, rows, layers
):
    each = rows // 2
    stride = gath_ref.shape[0] // count
    for i in range(count):
        tree_ref[i // 2, (i % 2) * each : (i % 2 + 1) * each] = gath_ref[
            i * stride : i * stride + each
        ]
    offsets = [0]
    for level in range(1, levels):
        base, size = offsets[-1] + (count >> level), count >> (level + 1)
        pairs = tree_ref[offsets[-1] : base].reshape((size, 2) + tree_ref.shape[1:])
        tree_ref[base : base + size] = pairs[:, 0] + pairs[:, 1]
        offsets.append(base)
    scaled = [
        pack(gamma_ref[level], fold) * (1.0 / (layers * 2.0 ** (level + 1)) ** 0.5)
        for level in range(levels)
    ]
    me = lax.axis_index(AXIS)
    coarse = []
    for shift in (-1, 0, 1):
        who = jnp.clip(me + shift, 0, count - 1)
        total = scaled[0] * tree_ref[offsets[0] + (who >> 1)]
        for level in range(1, levels):
            total = total + scaled[level] * tree_ref[offsets[level] + (who >> (level + 1))]
        if shift:
            total = total * (me + shift == who).astype(F32)
        coarse.append(unpack(total, fold))
    for i, block in enumerate(coarse):
        out_ref[i * block.shape[0] : (i + 1) * block.shape[0], : block.shape[1]] = block


def fill_spreads(coarse_ref, by_ref, bz_ref, spread_ref):
    ky = by_ref.shape[0]
    back_high, back_low = halves(
        dot3(halves(coarse_ref[: 3 * ky, : bz_ref.shape[0]]), halves(bz_ref[...]))
    )
    by_high, by_low = halves(by_ref[...])
    left = jnp.concatenate([by_high, by_high, by_low], axis=0)
    for i in range(spread_ref.shape[0]):
        high, low = (part[i * ky : (i + 1) * ky] for part in (back_high, back_low))
        right = jnp.concatenate([high, low, high], axis=0)
        spread_ref[i] = lax.dot_general(left, right, TN, preferred_element_type=F32)


PAD = 8


def tiles_of(ref):
    return ref.shape[-1] // LANES


def columns(j):
    return slice(j * LANES, (j + 1) * LANES)


def fill_tiles(tiled_ref, index, tile, j):
    ny = tile.shape[0]
    tiled_ref[index, j, PAD : PAD + ny] = tile


def clear_pads(tiled_ref):
    layers, tiles, full, _ = tiled_ref.shape
    zero = jnp.zeros((PAD, LANES), F32)
    for x in range(1, layers - 1):
        for j in range(tiles):
            tiled_ref[x, j, :PAD] = zero
            tiled_ref[x, j, full - PAD :] = zero


def stencil(tiled_ref, sigma_ref, wind_ref, x, first, rows, emit):
    tiles = tiled_ref.shape[1]
    lane = lax.broadcasted_iota(jnp.int32, (rows, LANES), 1)
    top = PAD + first
    here = [tiled_ref[x + 1, j, top : top + rows] for j in range(tiles)]
    up = [pltpu.roll(h, LANES - 1, 1) for h in here] + [jnp.zeros_like(here[0])]
    down = [jnp.zeros_like(here[0])] + [pltpu.roll(h, 1, 1) for h in here]
    for j in range(tiles):
        prev = tiled_ref[x, j, top : top + rows]
        after = tiled_ref[x + 2, j, top : top + rows]
        beside = (
            (after + prev)
            + (tiled_ref[x + 1, j, top - 1 : top - 1 + rows] + tiled_ref[x + 1, j, top + 1 : top + 1 + rows])
            + (
                jnp.where(lane == LANES - 1, up[j + 1], up[j])
                + jnp.where(lane == 0, down[j], down[j + 1])
            )
        )
        at = (x, slice(first, first + rows), columns(j))
        value = (6.0 + sigma_ref[at]) * here[j] - beside + wind_ref[at] * (after - prev)
        emit(at, value)


def rows_sum(x):
    return jnp.sum(x.reshape(x.shape[0] // 8, 8, LANES), axis=0)


def full_sum(x):
    return jnp.sum(x, axis=(0, 1), keepdims=True)


def even_here():
    return lax.rem(lax.axis_index(AXIS), 2) == 0


def send_edges(local_ref, pair_ref, odd_ref):
    layers, ny, _ = local_ref.shape
    even = even_here()
    pair_ref[:ny] = local_ref[jnp.where(even, layers - 1, 0)]
    odd_ref[0] = local_ref[jnp.where(even, 0, layers - 1)]


def send_proj(packed, scalars, pair_ref, ny):
    each = packed.shape[0] // 2
    parts = [packed[:each], packed[each:]]
    if scalars:
        parts.append(jnp.concatenate(scalars + [jnp.zeros((each - len(scalars), LANES), F32)], axis=0))
    used = sum(p.shape[1] for p in parts)
    if used < pair_ref.shape[1]:
        parts.append(jnp.zeros((each, pair_ref.shape[1] - used), F32))
    pair_ref[ny:] = jnp.concatenate(parts, axis=1)


def first_kernel(
    r_hbm, inv_hbm, local_ref, summed_ref, odd_ref, high_ref, low_ref, rr_ref, r_ref,
    inv_ref, sems
):
    layers, ny, nz = r_ref.shape
    half = nz // 2
    moves = [(inv_hbm.at[0, :half], inv_ref.at[:half])]
    moves += [(r_hbm.at[x], r_ref.at[x]) for x in range(layers)]
    moves += [(inv_hbm.at[0, half:], inv_ref.at[half:])]
    loads = [pltpu.make_async_copy(*move, sems.at[i]) for i, move in enumerate(moves)]
    for load in loads:
        load.start()
    loads[0].wait()
    upper = halves(inv_ref[:half])
    high_ref[:half], low_ref[:half] = upper
    total = jnp.zeros((8, LANES), F32)
    for x in range(0, layers, STEP):
        for load in loads[x + 1 : x + 1 + STEP]:
            load.wait()
        lines = r_ref[x : x + STEP, :, :half].reshape(STEP * ny, half)
        local_ref[x : x + STEP] = dot3(halves(lines), upper).reshape(STEP, ny, nz)
        for y in range(x, x + STEP):
            for j in range(tiles_of(r_ref)):
                r = r_ref[y, :, columns(j)]
                total = total + rows_sum(r * r)
                summed_ref[:, columns(j)] = r if y == 0 else summed_ref[:, columns(j)] + r
    rr_ref[:8] = total
    loads[layers + 1].wait()
    lower = halves(inv_ref[half:])
    high_ref[half:], low_ref[half:] = lower
    for x in range(0, layers, STEP):
        lines = r_ref[x : x + STEP, :, half:].reshape(STEP * ny, half)
        local_ref[x : x + STEP] += dot3(halves(lines), lower).reshape(STEP, ny, nz)
    odd_ref[0] = local_ref[jnp.where(even_here(), 0, layers - 1)]


def project_kernel(summed_ref, local_ref, by_ref, bz_ref, pair_ref, *, fold):
    layers, ny, _ = local_ref.shape
    pair_ref[:ny] = local_ref[jnp.where(even_here(), layers - 1, 0)]
    send_proj(project(summed_ref[...], by_ref[...], bz_ref[...], fold), [], pair_ref, ny)


def halo_of(even_ref, odd_ref, j):
    ny = odd_ref.shape[1]
    even = even_here()
    pair = even_ref[:ny, columns(j)]
    odd = odd_ref[0, :, columns(j)]
    return jnp.where(even, odd, pair), jnp.where(even, pair, odd)


def middle_kernel(
    coarse_ref, local_ref, even_ref, odd_ref, r_ref, sigma_ref, wind_ref, by_ref, bz_ref,
    high_ref, low_ref, rr_ref,
    z_ref, w_ref, pair2_ref, local2_ref, odd2_ref, spread_ref, *, fold,
):
    layers, ny, _ = r_ref.shape
    fill_spreads(coarse_ref, by_ref, bz_ref, spread_ref)
    clear_pads(z_ref)
    for j in range(tiles_of(r_ref)):
        before, after = halo_of(even_ref, odd_ref, j)
        fill_tiles(z_ref, 0, spread_ref[0, :, columns(j)] + before, j)
        fill_tiles(z_ref, layers + 1, spread_ref[2, :, columns(j)] + after, j)
        own = spread_ref[1, :, columns(j)]
        for x in range(layers):
            fill_tiles(z_ref, x + 1, local_ref[x, :, columns(j)] + own, j)
    sums = [rr_ref[:8]] + [jnp.zeros((8, LANES), F32)] * 2

    def emit(at, w):
        w_ref[at] = w
        sums[1] = sums[1] + rows_sum(r_ref[at] * w)
        sums[2] = sums[2] + rows_sum(w * w)

    for x in range(layers):
        for first in range(0, ny, CHUNK):
            stencil(z_ref, sigma_ref, wind_ref, x, first, CHUNK, emit)
        if x % 2:
            both = halves(w_ref[x - 1 : x + 1].reshape(2 * ny, -1))
            product = dot3(both, (high_ref[...], low_ref[...]))
            local2_ref[x - 1 : x + 1] = product.reshape(2, ny, -1)
    summed = w_ref[0]
    for x in range(1, layers):
        summed = summed + w_ref[x]
    packed = project(summed, by_ref[...], bz_ref[...], fold)
    send_proj(packed, [jnp.sum(s, axis=0, keepdims=True) for s in sums], pair2_ref, ny)
    send_edges(local2_ref, pair2_ref, odd2_ref)


def lane_of(row, which):
    lane = lax.broadcasted_iota(jnp.int32, row.shape, 1)
    return full_sum(jnp.where(lane == which, row, 0.0))


def first_scalars(gath_ref, rows):
    size = rows // 2 + 1
    row = gath_ref[size - 1 : size]
    for i in range(2, gath_ref.shape[0] // size, 2):
        row = row + gath_ref[(i + 1) * size - 1 : (i + 1) * size]
    rr, rw, ww = (lane_of(row, i) for i in range(3))
    inv_rr = 1.0 / rr
    beta = jnp.sqrt(rr)
    h11 = rw * inv_rr
    h21 = jnp.sqrt(ww * inv_rr - h11 * h11)
    return beta, h11, h21


def last_kernel(
    gath_ref, coarse_ref, local_ref, even_ref, odd_ref, r_ref, z_ref, w_ref,
    sigma_ref, wind_ref, by_ref, bz_ref, z2_ref, u_ref, out_ref, known_ref, spread_ref, *, rows,
):
    layers, ny, _ = r_ref.shape
    fill_spreads(coarse_ref, by_ref, bz_ref, spread_ref)
    beta, h11, h21 = first_scalars(gath_ref, rows)
    scale = 1.0 / (h21 * beta)
    minus = scale * h11
    clear_pads(z2_ref)

    def combine(index, image, j):
        old = z_ref[index, j, PAD : PAD + ny]
        fill_tiles(z2_ref, index, scale * image - minus * old, j)

    for j in range(tiles_of(r_ref)):
        before, after = halo_of(even_ref, odd_ref, j)
        combine(0, spread_ref[0, :, columns(j)] + before, j)
        combine(layers + 1, spread_ref[2, :, columns(j)] + after, j)
        own = spread_ref[1, :, columns(j)]
        for x in range(layers):
            combine(x + 1, local_ref[x, :, columns(j)] + own, j)
    sums = [jnp.zeros((8, LANES), F32)] * 3

    def emit(at, u):
        u_ref[at] = u
        for i, product in enumerate((r_ref[at] * u, w_ref[at] * u, u * u)):
            sums[i] = sums[i] + rows_sum(product)

    for x in range(layers):
        for first in range(0, ny, CHUNK):
            stencil(z2_ref, sigma_ref, wind_ref, x, first, CHUNK, emit)
    lane = lax.broadcasted_iota(jnp.int32, (1, LANES), 1)
    a, b, c = (full_sum(s) for s in sums)
    b = scale * b - minus * a
    row = jnp.where(lane == 0, a, jnp.where(lane == 1, b, jnp.where(lane == 2, c, 0.0)))
    out_ref[...] = jnp.broadcast_to(row, out_ref.shape)
    for i, value in enumerate((beta, h11, h21)):
        known_ref[8 * i : 8 * i + 8] = jnp.broadcast_to(value, (8, LANES))


def finish_kernel(
    sums_ref, known_ref, r_ref, z_ref, w_ref, z2_ref, u_ref, sol_hbm, res_hbm,
    sol_ref, res_ref, sems,
):
    layers, ny, _ = r_ref.shape
    beta, h11, h21 = (known_ref[8 * i : 8 * i + 1, :1] for i in range(3))
    sums = jnp.sum(sums_ref[...], axis=0, keepdims=True)
    h12 = lane_of(sums, 0) / beta
    h22 = lane_of(sums, 1)
    h32 = jnp.sqrt(lane_of(sums, 2) - h12 * h12 - h22 * h22)
    m11 = h11 * h11 + h21 * h21
    m12 = h11 * h12 + h21 * h22
    m22 = h12 * h12 + h22 * h22 + h32 * h32
    q_one = h11 * beta
    q_two = h12 * beta
    determ = m11 * m22 - m12 * m12
    y_one = (m22 * q_one - m12 * q_two) / determ / beta
    y_two = (m11 * q_two - m12 * q_one) / determ
    stores = []
    for x in range(layers):
        for j in range(tiles_of(r_ref)):
            inside = (x + 1, j, slice(PAD, PAD + ny))
            sol_ref[x, :, columns(j)] = y_one * z_ref[inside] + y_two * z2_ref[inside]
        res_ref[x] = r_ref[x] - (y_one * w_ref[x] + y_two * u_ref[x])
        for i, (src, dst) in enumerate(((sol_ref, sol_hbm), (res_ref, res_hbm))):
            store = pltpu.make_async_copy(src.at[x], dst.at[x], sems.at[2 * x + i])
            store.start()
            stores.append(store)
    for store in stores:
        store.wait()


def call(kernel, outs, args, scratch=(), flops=0, hbm=(), far_out=False, limit=24):
    vmem = pl.BlockSpec(memory_space=pltpu.VMEM)
    far = pl.BlockSpec(memory_space=pltpu.HBM)
    outs = [s if isinstance(s, jax.ShapeDtypeStruct) else jax.ShapeDtypeStruct(s, F32) for s in outs]
    return pl.pallas_call(
        kernel,
        out_shape=outs,
        in_specs=[far if i in hbm else vmem for i in range(len(args))],
        out_specs=[far if far_out else vmem] * len(outs),
        scratch_shapes=[pltpu.VMEM(s, F32) if isinstance(s, tuple) else s for s in scratch],
        compiler_params=pltpu.CompilerParams(vmem_limit_bytes=limit << 20),
        cost_estimate=pl.CostEstimate(flops=flops, bytes_accessed=0, transcendentals=0),
    )(*args)


def exchange(block):
    return lax.all_to_all(block, AXIS, 0, 0, tiled=True)


def on_device(right_side, sigma, wind, local_inverse, basis_y, basis_z, gamma):
    count = lax.axis_size(AXIS)
    levels = count.bit_length() - 1
    layers, ny, nz = right_side.shape
    ky, kz = basis_y.shape[1], basis_z.shape[1]
    fold = fold_of(ky, kz)
    rows, width = ky // fold, kz * fold
    field = (layers, ny, nz)
    edge = (1, ny, nz)
    pairs = [(i, i ^ 1) for i in range(count)]
    others = [(i, i + 1) for i in range(1, count - 1, 2)]
    others = others + [(j, i) for i, j in others]
    matmul = 6 * layers * ny * nz * nz
    by, bz = basis_y.T, basis_z.T
    each = rows // 2
    pair = (ny + each, nz)
    tiled = (layers + 2, nz // LANES, ny + 2 * PAD, LANES)

    def round_of(sent, odd, extra):
        got = lax.ppermute(sent, AXIS, pairs)
        odd = lax.ppermute(odd, AXIS, others)
        size = each + extra
        (block,) = call(
            functools.partial(join_kernel, rows=rows, width=width, extra=extra),
            [(count * size, width)], (got, sent), flops=matmul // 16,
        )
        block = exchange(block.reshape(count * size, 1, width)).reshape(count * size, width)
        (coarse,) = call(
            functools.partial(
                coarse_kernel, fold=fold, levels=levels, count=count, rows=rows, layers=layers
            ),
            [(-(-3 * ky // 32) * 32, LANES)], (block, gamma), [(count, rows, width)],
            flops=matmul // 16,
        )
        return block, coarse, got, odd

    square = jax.ShapeDtypeStruct((nz, nz), BF16)
    local, summed, odd, high, low, rr, r = call(
        first_kernel, [field, (ny, nz), edge, square, square, (32, LANES), field],
        (right_side, local_inverse),
        [(nz, nz), pltpu.SemaphoreType.DMA((layers + 2,))],
        flops=matmul, hbm=(0, 1), limit=FIRST_LIMIT,
    )
    (sent,) = call(
        functools.partial(project_kernel, fold=fold), [pair],
        (summed, local, by, bz), flops=matmul // 8,
    )
    _, coarse, got, odd = round_of(sent, odd, 0)
    z, w, sent, local, odd = call(
        functools.partial(middle_kernel, fold=fold),
        [tiled, field, pair, field, edge],
        (coarse, local, got, odd, r, sigma, wind, by, bz, high, low, rr),
        [(3, ny, nz)], flops=2 * matmul,
    )
    gathered, coarse, got, odd = round_of(sent, odd, 1)
    z2, u, sent, known = call(
        functools.partial(last_kernel, rows=rows),
        [tiled, field, (count, LANES), (32, LANES)],
        (gathered, coarse, local, got, odd, r, z, w, sigma, wind, by, bz),
        [(3, ny, nz)], flops=matmul,
    )
    sums = exchange(sent)
    return call(
        finish_kernel, [field, field], (sums, known, r, z, w, z2, u),
        [field, field, pltpu.SemaphoreType.DMA((2 * layers,))],
        flops=matmul // 8, far_out=True,
    )


def solution(mesh):
    placed = (P(AXIS, None, None),) * 4 + (P(),) * 3
    return jax.shard_map(
        lambda *args: tuple(on_device(*args)),
        mesh=mesh,
        in_specs=placed,
        out_specs=(P(AXIS, None, None), P(AXIS, None, None)),
        check_vma=False,
    )
```
